512 devices in a mesh: ga: 2 (over y), gx: 16 (over z), gy: 8 (over x), col: 2 (over core).
Axes of the slice: x: 8, y: 2, z: 16, core: 2. Of those that a mesh axis runs over, the one named last changes fastest.
The devices are a block of a 8x8x16 slice.
Arguments:
- pair_rep: bfloat16 [2, 640, 640, 128], P('ga', 'gx', 'gy'), parts along dimension 0, may hold values from -6 to 6
- pair_mask: int32 [2, 640, 640], P('ga', 'gx', 'gy'), parts along dimension 0, may hold values 0 or 1
- amax_history: float32 [2, 128], P(None, 'col'), may hold values from 0.3 to 3
- in_gain: float32 [128], replicated, may hold values from 0.5 to 1.5
- in_bias: float32 [128], replicated, may hold values from -3 to 3
- proj_weight: bfloat16 [128, 4, 128], P(None, None, 'col'), may hold values from -0.5 to 0.5
- gate_weight: bfloat16 [128, 128], P(None, 'col'), may hold values from -0.5 to 0.5
- out_gain: float32 [128], replicated, may hold values from 0.5 to 1.5
- out_bias: float32 [128], replicated, may hold values from -3 to 3
- out_weight: bfloat16 [128, 128], P(None, 'col'), may hold values from -0.5 to 0.5
Outputs:
- update: bfloat16 [2, 640, 640, 128], P('ga', 'gx', 'gy', 'col'), parts along dimension 0
- new_amax: float32 [4, 128], P('ga', 'col'), parts along dimension 0
The draws below stay inside these ranges and needn't reach their ends.
There are 2 independent parts, one for each index of `ga`. The reference program is written for one: setup_inputs(seed, part) draws one part's arguments, and reference() takes and returns one part's arrays. A program takes and returns all parts, laid end to end along the dimension named above; an argument that names none is the same for every part. Nothing has to cross between parts.
All inputs are finite; a program needn't handle non-finite values. No bound on the sum of `pair_mask` on one device may be relied on, other than what follows from the above.
Results may differ from the reference program's by a relative error of at most 0.0065.
Values may be sent and summed in bfloat16 or wider, within the bound.
No kernel may reach another device: no remote copies, remote signals or barrier semaphores. Data moves between devices by JAX's collectives and lax.ppermute only.
A program may use at most 128 MiB of HBM per device.

```python
import math
import jax
import jax.numpy as jnp
from jax import lax

C = 128
CROPS = 1
N = 640


def place_ends(result, stream_key, low, top_value):
    longest = result.shape.index(max(result.shape))
    spots = []
    for shift in (0, 1):
        where = [jax.random.randint(jax.random.fold_in(stream_key, axis), (), 0, length) for axis, length in enumerate(result.shape)]
        where[longest] = (where[longest] + shift) % result.shape[longest]
        spots.append(tuple(where))
    return result.at[spots[0]].set(low).at[spots[1]].set(top_value)


def levels(key, shape, cuts, low, largest):
    level, own = 1.0, jax.random.fold_in(key, 6)
    for axis_at, blocks in cuts:
        heights = jnp.exp(jax.random.uniform(jax.random.fold_in(own, axis_at), (blocks,), jnp.float32, low / len(cuts), largest / len(cuts)))
        level = level * jnp.repeat(heights, shape[axis_at] // blocks).reshape([-1 if axis == axis_at else 1 for axis in range(len(shape))])
    return level


def scatter_about(own_key, extent, scale, reach, pieces=(), held_as=jnp.bfloat16):
    result = scale * jax.random.normal(own_key, extent, jnp.float32)
    if pieces:
        result = result * levels(own_key, extent, pieces, -0.22, 0.18)
    return jnp.clip(result, -reach, reach).astype(held_as)


def setup_inputs(seed: int = 0, part: int = 0) -> dict:
    seeds = jax.random.split(jax.random.key(seed), 11)
    part_keys = jax.random.split(jax.random.fold_in(seeds[10], part), 11)
    pair_rep = scatter_about(part_keys[0], (CROPS, N, N, C), 1.0, 6.0, ((1, 16), (2, 8)))
    pair_mask = place_ends((jax.random.randint(part_keys[1], (CROPS, N, N), 0, 10) < 9).astype(jnp.int32), jax.random.fold_in(part_keys[1], 1), 0, 1)
    amax_history = jnp.clip(jnp.exp(math.log(3.0) - 2.3025851 * jax.random.uniform(seeds[2], (2, C), jnp.float32) ** levels(seeds[2], (2, C), ((1, 2),), -0.2, 0.2)), 0.3, 3.0)
    in_gain = jnp.clip(1.0 + 0.1 * jax.random.normal(seeds[3], (C,), jnp.float32), 0.5, 1.5)
    in_bias = scatter_about(seeds[4], (C,), 0.5, 3.0, (), jnp.float32)
    proj_weight = scatter_about(seeds[5], (C, 4, C), C ** -0.5, 0.5, ((2, 2),))
    gate_weight = scatter_about(seeds[6], (C, C), C ** -0.5, 0.5, ((1, 2),))
    out_gain = jnp.clip(1.0 + 0.1 * jax.random.normal(seeds[7], (C,), jnp.float32), 0.5, 1.5)
    out_bias = scatter_about(seeds[8], (C,), 0.5, 3.0, (), jnp.float32)
    out_weight = scatter_about(seeds[9], (C, C), C ** -0.5, 0.5, ((1, 2),))
    return {"pair_rep": pair_rep, "pair_mask": pair_mask, "amax_history": amax_history, "in_gain": in_gain, "in_bias": in_bias, "proj_weight": proj_weight, "gate_weight": gate_weight, "out_gain": out_gain, "out_bias": out_bias, "out_weight": out_weight}


epsilon = 1e-05
format_limit = 448.0

def layer_norm(values, gain, bias):
    average = lax.optimization_barrier(jnp.mean(values, axis=-1, keepdims=True))
    spread = lax.optimization_barrier(jnp.mean(jnp.square(values - average), axis=-1, keepdims=True))
    return (values - average) * lax.rsqrt(spread + epsilon) * gain + bias

def one_crop(crop_rep, crop_mask, amax_history, in_gain, in_bias, proj_weight, gate_weight, out_gain, out_bias, out_weight):
    normed = layer_norm(crop_rep.astype(jnp.float32), in_gain, in_bias).astype(jnp.bfloat16)
    flat = normed.reshape(N * N, C)
    masking = crop_mask.astype(jnp.float32).reshape(N * N, 1)

    def project(which):
        return jnp.dot(flat, proj_weight[:, which, :], preferred_element_type=jnp.float32)
    left_proj = masking * jax.nn.sigmoid(project(1)) * project(0)
    right_proj = masking * jax.nn.sigmoid(project(3)) * project(2)
    crop_amax = jnp.stack([lax.optimization_barrier(jnp.max(jnp.abs(left_proj), axis=0)), lax.optimization_barrier(jnp.max(jnp.abs(right_proj), axis=0))])
    scales = amax_history / format_limit
    left_q = jnp.clip(left_proj / scales[0], -format_limit, format_limit).astype(jnp.bfloat16).reshape(N, N, C)
    right_q = jnp.clip(right_proj / scales[1], -format_limit, format_limit).astype(jnp.bfloat16).reshape(N, N, C)
    products = jnp.einsum('ikc,jkc->ijc', left_q.astype(jnp.float32), right_q.astype(jnp.float32))
    triangle = (products * (scales[0] * scales[1])).astype(jnp.bfloat16)
    tnorm = layer_norm(triangle.astype(jnp.float32), out_gain, out_bias).astype(jnp.bfloat16)
    gating = jax.nn.sigmoid(jnp.dot(flat, gate_weight, preferred_element_type=jnp.float32))
    mixing = jnp.dot(tnorm.reshape(N * N, C), out_weight, preferred_element_type=jnp.float32)
    update = (gating * mixing).astype(jnp.bfloat16).reshape(N, N, C)
    return (update, crop_amax)

def reference(pair_rep, pair_mask, amax_history, in_gain, in_bias, proj_weight, gate_weight, out_gain, out_bias, out_weight):
    updates = []
    maxima = []
    for crop in range(CROPS):
        update, crop_amax = one_crop(pair_rep[crop], pair_mask[crop], amax_history, in_gain, in_bias, proj_weight, gate_weight, out_gain, out_bias, out_weight)
        updates.append(update)
        maxima.append(crop_amax)
    new_amax = maxima[0]
    for crop_amax in maxima[1:]:
        new_amax = jnp.maximum(new_amax, crop_amax)
    return (jnp.stack(updates), new_amax)
```

```python
import functools

import jax
import jax.numpy as jnp
from jax import lax
from jax.experimental import pallas as pl
from jax.experimental.pallas import tpu as pltpu
from jax.sharding import PartitionSpec as P

epsilon = 1e-05
format_limit = 448.0
LANES = 128
F32 = jnp.float32
BF16 = jnp.bfloat16


def lane_round(size):
    return -(-size // LANES) * LANES


def normed_rows(rows, gain, bias):
    average = jnp.mean(rows, axis=-1, keepdims=True)
    spread = jnp.mean(jnp.square(rows - average), axis=-1, keepdims=True)
    return ((rows - average) * lax.rsqrt(spread + epsilon) * gain + bias).astype(BF16)


def one_hot_rows(channels, parity, dtype=BF16):
    row = lax.broadcasted_iota(jnp.int32, (2 * channels, channels), 0)
    col = lax.broadcasted_iota(jnp.int32, (2 * channels, channels), 1)
    return jnp.where(row == 2 * col + parity, 1.0, 0.0).astype(dtype)


def one_hot_cols(channels, parity):
    row = lax.broadcasted_iota(jnp.int32, (channels, 2 * channels), 0)
    col = lax.broadcasted_iota(jnp.int32, (channels, 2 * channels), 1)
    return jnp.where(col == 2 * row + parity, 1.0, 0.0).astype(BF16)


def nn(left, right):
    return jnp.dot(left, right, preferred_element_type=F32)


def nt(left, right):
    return lax.dot_general(left, right, (((1,), (1,)), ((), ())), preferred_element_type=F32)


def split_parts(values):
    high = values.astype(BF16).astype(F32)
    middle = (values - high).astype(BF16).astype(F32)
    return high, middle, values - high - middle


def project_kernel(
    half_ref, rep_ref, mask_ref, weight_ref, inverse_ref, gain_ref, bias_ref, out_ref, near, far, proj
):
    rows, cols, channels = rep_ref.shape
    deep = rows // 4
    span = deep * cols
    wide = near.shape[0]
    shift = span - (wide - LANES)
    half = half_ref[0]
    gain, bias = gain_ref[...], bias_ref[...]
    near[pl.ds(span, wide - span), :] = jnp.zeros((wide - span, 2 * channels), BF16)
    far[pl.ds(0, shift), :] = jnp.zeros((shift, 2 * channels), BF16)
    far[pl.ds(shift + span, wide - span - shift), :] = jnp.zeros((wide - span - shift, 2 * channels), BF16)
    for part in range(2):
        for at in range(deep):
            block = rep_ref[half * (2 * deep) + part * deep + at].astype(F32)
            block = normed_rows(block, gain, bias)
            near[at * cols : (at + 1) * cols, part * channels : (part + 1) * channels] = block
            far[shift + at * cols : shift + (at + 1) * cols, part * channels : (part + 1) * channels] = block
    even, odd = one_hot_rows(channels, 0), one_hot_rows(channels, 1)
    for which in range(4):
        weight = jnp.concatenate([weight_ref[0, which], weight_ref[1, which]], axis=0)
        weight = jnp.concatenate([nn(even, weight), nn(odd, weight)], axis=1).astype(BF16)
        proj[which] = nt(weight, (near if which < 2 else far)[...])
    masks = mask_ref[...].astype(F32)
    masks = jnp.where(half == 0, masks[: 2 * deep], masks[2 * deep :])
    pieces = [
        jnp.concatenate([masks[at : at + 1], masks[deep + at : deep + at + 1]], axis=0)
        for at in range(deep)
    ]
    zeros = jnp.zeros((2, wide - span), F32)
    mask_near = jnp.concatenate([*pieces, zeros], axis=1)
    mask_far = pltpu.roll(jnp.concatenate([mask_near] * 4, axis=0), shift, 1)
    mask_near = jnp.concatenate([mask_near] * 8, axis=0)
    mask_far = jnp.concatenate([mask_far] * 2, axis=0)
    lane = lax.broadcasted_iota(jnp.int32, (16, LANES), 1)
    first = shift + span - (wide - LANES)

    def step(at, carry):
        rows_at = pl.ds(pl.multiple_of(at * 16, 16), 16)
        left = mask_near * jax.nn.sigmoid(proj[1, rows_at, :]) * proj[0, rows_at, :]
        right = mask_far * jax.nn.sigmoid(proj[3, rows_at, :]) * proj[2, rows_at, :]
        left_max = jnp.max(jnp.abs(left), axis=1, keepdims=True)
        right_max = jnp.max(jnp.abs(right), axis=1, keepdims=True)
        inverse = inverse_ref[rows_at, :]
        left = jnp.clip(left * inverse[:, 0:1], -format_limit, format_limit)
        right = jnp.clip(right * inverse[:, 1:2], -format_limit, format_limit)
        edge = wide - LANES
        out_ref[rows_at, 0:edge] = left[:, :edge].astype(BF16)
        out_ref[rows_at, edge:wide] = (left[:, edge:] + right[:, :LANES]).astype(BF16)
        out_ref[rows_at, wide : wide + edge - LANES] = right[:, LANES:edge].astype(BF16)
        last = right[:, edge:]
        for place, part in enumerate((*split_parts(left_max), *split_parts(right_max))):
            last = jnp.where(lane == first + place, part, last)
        out_ref[rows_at, wide + edge - LANES : wide + edge] = last.astype(BF16)
        return carry

    lax.fori_loop(0, 2 * channels // 16, step, 0)


def gate_kernel(
    rep_ref, gate_ref, weight_ref, gain_ref, bias_ref, gating_ref, mixer_ref, order_ref, near
):
    rows, cols, channels = rep_ref.shape
    deep = rows // 4
    span = deep * cols
    outs = gate_ref.shape[0]
    gain, bias = gain_ref[...], bias_ref[...]
    blank = jnp.zeros((outs, channels), BF16)
    gate = gate_ref[...]
    wide_gate = jnp.concatenate(
        [jnp.concatenate([gate, blank], axis=1), jnp.concatenate([blank, gate], axis=1)], axis=0
    )
    near[span:, :] = jnp.zeros((near.shape[0] - span, 2 * channels), BF16)
    for half in range(2):
        for part in range(2):
            for at in range(deep):
                block = rep_ref[half * (2 * deep) + part * deep + at].astype(F32)
                near[at * cols : (at + 1) * cols, part * channels : (part + 1) * channels] = normed_rows(
                    block, gain, bias
                )
        gating_ref[half] = jax.nn.sigmoid(nt(wide_gate, near[...]))
    weight = weight_ref[...]
    mixer_ref[0:outs, :] = nn(weight, one_hot_cols(channels, 0)).astype(BF16)
    mixer_ref[outs:, :] = nn(weight, one_hot_cols(channels, 1)).astype(BF16)
    count, lanes = order_ref.shape
    per_half = count // 2
    per_at = per_half // deep
    pairs = cols // rows
    step = 32
    for start in range(0, count, step):
        row = start + lax.broadcasted_iota(jnp.int32, (step, 1), 0)
        half_at = start // per_half
        deep_at = (start % per_half) // per_at
        block = (row - half_at * per_half - deep_at * per_at) >> 1
        part = row & 1
        target = (block // pairs) * LANES + (block % pairs) * rows + half_at * 2 * deep + part * deep + deep_at
        lane = lax.broadcasted_iota(jnp.int32, (step, lanes), 1)
        order_ref[start : start + step, :] = jnp.where(lane == target, 1.0, 0.0).astype(BF16)


def triangle_kernel(
    scale_ref, own_ref, both_ref, order_ref, out_ref, left, right, moved, *, groups, deep, cols
):
    rows, wide = both_ref.shape[1:]
    block = rows // groups
    span = deep * cols
    first = span - (wide - LANES)
    used = lax.broadcasted_iota(jnp.int32, (block, LANES), 1) < cols
    none = jnp.zeros((block, LANES), BF16)

    def window(ref, group, start):
        base = start // LANES * LANES
        rows_at = pl.ds(group * block, block)
        if start == base:
            return ref[rows_at, base : base + LANES]
        return ref[rows_at, base : base + 2 * LANES][:, start - base : start - base + LANES]

    for group in range(groups):
        for at in range(deep):
            piece = window(own_ref, group, at * cols)
            left[at * block : (at + 1) * block, group * LANES : (group + 1) * LANES] = jnp.where(used, piece, none)
            for other in range(2):
                place = (other * deep + at) * block
                right[place : place + block, group * LANES : (group + 1) * LANES] = window(
                    both_ref.at[other], group, first + at * cols
                )
    products = nt(left[...], right[...]) * scale_ref[0]
    moved[...] = nn(products.astype(BF16), order_ref[...]).astype(BF16)
    lane = lax.broadcasted_iota(jnp.int32, (8, LANES), 1)
    first = first + span - (wide - LANES)
    best = None
    for other in range(2):
        parts = both_ref[other, :, wide - LANES :].astype(F32)
        total = parts + pltpu.roll(parts, LANES - 1, 1) + pltpu.roll(parts, LANES - 2, 1)
        total = jnp.max(total.reshape(rows // 8, 8, LANES), axis=0)
        best = total if best is None else jnp.maximum(best, total)
    best = jnp.broadcast_to(jnp.max(best, axis=0, keepdims=True), (8, LANES))
    goal = span % LANES
    tail = jnp.zeros((8, LANES), F32)
    for place, part in enumerate(split_parts(best)):
        turned = pltpu.roll(part, (goal + place - first) % LANES, 1)
        tail = jnp.where((lane == goal + place) | (lane == goal + place + 3), turned, tail)
    tail = tail[0:1, goal:].astype(BF16)
    tail = jnp.broadcast_to(tail.astype(F32), (block, LANES - goal)).astype(BF16)
    for group in range(groups):
        pieces = [
            moved[at * block : (at + 1) * block, group * LANES : group * LANES + cols] for at in range(deep)
        ]
        out_ref[group * block : (group + 1) * block, :] = jnp.concatenate([*pieces, tail], axis=1)


def finish_kernel(
    half_ref, both_ref, gating_ref, mixer_ref, gain_ref, bias_ref, update_ref, amax_ref, mixed, *, deep, cols
):
    rows, wide = both_ref.shape[1:]
    channels = rows // 2
    outs = update_ref.shape[1]
    span = deep * cols
    gain, bias = gain_ref[...], bias_ref[...]
    mixer = mixer_ref[...]

    def per_part(values):
        total = jnp.sum(values, axis=0)
        total = total + pltpu.roll(total, 4, 0)
        total = total + pltpu.roll(total, 2, 0)
        return total * (1.0 / channels)

    for half in range(2):
        for start in range(0, wide, LANES):
            values = both_ref[half, :, start : start + LANES].astype(F32).reshape(rows // 8, 8, LANES)
            values = values - per_part(values)[None]
            spread = per_part(jnp.square(values))
            values = (values * lax.rsqrt(spread + epsilon)[None]).reshape(rows, LANES)
            tnorm = (values * gain + bias).astype(BF16)
            mixing = nn(mixer, tnorm)
            mixed[:, start : start + LANES] = (gating_ref[half, :, start : start + LANES] * mixing).astype(BF16)
        for part in range(2):
            for at in range(deep):
                place = half * 2 * deep + part * deep + at
                update_ref[place] = mixed[part * outs : (part + 1) * outs, at * cols : (at + 1) * cols]
    last = both_ref[0, :, wide - LANES :]
    row = lax.broadcasted_iota(jnp.int32, (rows, outs), 0)
    col = lax.broadcasted_iota(jnp.int32, (rows, outs), 1)
    chosen = jnp.where(row == 2 * (col + half_ref[0] * outs), 1.0, 0.0).astype(BF16)
    sums = lax.dot_general(last, chosen, (((0,), (0,)), ((), ())), preferred_element_type=F32)
    goal = span % LANES
    amax_ref[0:1, :] = sums[goal : goal + 1] + sums[goal + 1 : goal + 2] + sums[goal + 2 : goal + 3]
    amax_ref[1:2, :] = sums[goal + 3 : goal + 4] + sums[goal + 4 : goal + 5] + sums[goal + 5 : goal + 6]


VMEM = pl.BlockSpec(memory_space=pltpu.VMEM)
SMEM = pl.BlockSpec(memory_space=pltpu.SMEM)


def on_device(
    pair_rep,
    pair_mask,
    amax_history,
    in_gain,
    in_bias,
    proj_weight,
    gate_weight,
    out_gain,
    out_bias,
    out_weight,
):
    rows, cols, channels = pair_rep.shape[1:]
    deep = rows // 4
    span = deep * cols
    wide = lane_round(span)
    groups, ranks = lax.axis_size("gy"), lax.axis_size("gx")
    chips = ("gy", "gx")
    assert groups * ranks == channels and lax.axis_size("col") == 2
    half = lax.axis_index("col").reshape(1).astype(jnp.int32)
    rep = pair_rep[0]
    gain, bias = in_gain[None, :], in_bias[None, :]

    weights = lax.all_gather(jnp.transpose(proj_weight, (1, 2, 0)), "col")
    history = jnp.transpose(lax.all_gather(amax_history, "col"), (1, 0, 2)).reshape(2, channels)
    scales = history / format_limit
    inverse = jnp.repeat((1.0 / scales).T, 2, axis=0)
    message = pl.pallas_call(
        project_kernel,
        name="project",
        out_shape=jax.ShapeDtypeStruct((2 * channels, 2 * wide - LANES), BF16),
        in_specs=[SMEM] + [VMEM] * 6,
        out_specs=VMEM,
        scratch_shapes=[
            pltpu.VMEM((wide, 2 * channels), BF16),
            pltpu.VMEM((wide, 2 * channels), BF16),
            pltpu.VMEM((4, 2 * channels, wide), F32),
        ],
    )(half, rep, pair_mask[0], weights, inverse, gain, bias)
    received = lax.all_to_all(
        message.reshape(channels, 2, -1), chips, split_axis=0, concat_axis=0, tiled=True
    )
    gating, mixer, order = pl.pallas_call(
        gate_kernel,
        name="gate",
        out_shape=(
            jax.ShapeDtypeStruct((2, channels, wide), F32),
            jax.ShapeDtypeStruct((channels, 2 * channels), BF16),
            jax.ShapeDtypeStruct((ranks * rows, groups * LANES), BF16),
        ),
        in_specs=[VMEM] * 5,
        out_specs=(VMEM,) * 3,
        scratch_shapes=[pltpu.VMEM((wide, 2 * channels), BF16)],
        cost_estimate=pl.CostEstimate(flops=20_000_000_000, bytes_accessed=3_000_000, transcendentals=0),
    )(rep, gate_weight.T, out_weight.T, gain, bias)
    received = received.reshape(2 * channels, -1)
    edge = wide - LANES
    both = lax.all_gather(received[:, edge:], "col")
    mine = lax.axis_index(chips)
    scale = lax.dynamic_slice(scales[0] * scales[1], (mine,), (1,))
    products = pl.pallas_call(
        functools.partial(triangle_kernel, groups=groups, deep=deep, cols=cols),
        name="triangle",
        out_shape=jax.ShapeDtypeStruct((2 * channels, wide), BF16),
        in_specs=[SMEM, VMEM, VMEM, VMEM],
        out_specs=VMEM,
        scratch_shapes=[
            pltpu.VMEM((ranks * rows // 2, groups * LANES), BF16),
            pltpu.VMEM((ranks * rows, groups * LANES), BF16),
            pltpu.VMEM((ranks * rows // 2, groups * LANES), BF16),
        ],
    )(scale, received, both, order)
    returned = lax.all_to_all(
        products.reshape(channels, 2, -1), chips, split_axis=0, concat_axis=0, tiled=True
    )
    both = lax.all_gather(returned.reshape(2 * channels, -1), "col")
    update, new_amax = pl.pallas_call(
        functools.partial(finish_kernel, deep=deep, cols=cols),
        name="finish",
        out_shape=(
            jax.ShapeDtypeStruct((rows, channels // 2, cols), BF16),
            jax.ShapeDtypeStruct((2, channels // 2), F32),
        ),
        in_specs=[SMEM] + [VMEM] * 5,
        out_specs=(VMEM,) * 2,
        scratch_shapes=[pltpu.VMEM((channels, wide), BF16)],
    )(half, both, gating, mixer, jnp.repeat(out_gain, 2)[:, None], jnp.repeat(out_bias, 2)[:, None])
    return (jnp.transpose(update, (0, 2, 1))[None], new_amax)


def solution(mesh):
    placed = (
        P("ga", "gx", "gy", None),
        P("ga", "gx", "gy"),
        P(None, "col"),
        P(),
        P(),
        P(None, None, "col"),
        P(None, "col"),
        P(),
        P(),
        P(None, "col"),
    )
    return jax.shard_map(
        on_device,
        mesh=mesh,
        in_specs=placed,
        out_specs=(P("ga", "gx", "gy", "col"), P("ga", "col")),
        check_vma=False,
    )
```

```python
import functools

import jax
import jax.numpy as jnp
from jax import lax
from jax.experimental import pallas as pl
from jax.experimental.pallas import tpu as pltpu
from jax.sharding import PartitionSpec as P

epsilon = 1e-05
format_limit = 448.0
LANES = 128
F32 = jnp.float32
BF16 = jnp.bfloat16


def lane_round(size):
    return -(-size // LANES) * LANES


def normed_rows(rows, gain, bias):
    average = jnp.mean(rows, axis=-1, keepdims=True)
    spread = jnp.mean(jnp.square(rows - average), axis=-1, keepdims=True)
    return ((rows - average) * lax.rsqrt(spread + epsilon) * gain + bias).astype(BF16)


def one_hot_rows(channels, parity, dtype=BF16):
    row = lax.broadcasted_iota(jnp.int32, (2 * channels, channels), 0)
    col = lax.broadcasted_iota(jnp.int32, (2 * channels, channels), 1)
    return jnp.where(row == 2 * col + parity, 1.0, 0.0).astype(dtype)


def one_hot_cols(channels, parity):
    row = lax.broadcasted_iota(jnp.int32, (channels, 2 * channels), 0)
    col = lax.broadcasted_iota(jnp.int32, (channels, 2 * channels), 1)
    return jnp.where(col == 2 * row + parity, 1.0, 0.0).astype(BF16)


def in_hbm(array):
    return pltpu.with_memory_space_constraint(array, pltpu.HBM)


def nn(left, right):
    return jnp.dot(left, right, preferred_element_type=F32)


def nt(left, right):
    return lax.dot_general(left, right, (((1,), (1,)), ((), ())), preferred_element_type=F32)


def split_parts(values):
    high = values.astype(BF16).astype(F32)
    middle = (values - high).astype(BF16).astype(F32)
    return high, middle, values - high - middle


def columns_of(rows, channels):
    parts = jnp.concatenate([*split_parts(rows), jnp.zeros_like(rows)], axis=0).astype(BF16)
    return columns_of_parts(parts, channels)


def columns_of_parts(parts, channels):
    both = (one_hot_rows(channels, 0, F32) + one_hot_rows(channels, 1, F32)).astype(BF16)
    columns = nt(both, parts)
    return columns[:, 0:2] + columns[:, 2:4] + columns[:, 4:6]


def prepare_kernel(
    half_ref,
    rep_hbm,
    mask_hbm,
    weight_hbm,
    history_hbm,
    gain_hbm,
    bias_hbm,
    packed_ref,
    near,
    far,
    masks_ref,
    rep_ref,
    mask_ref,
    weight_ref,
    history_ref,
    gain_ref,
    bias_ref,
    sems,
):
    which, outs, channels = weight_ref.shape
    held, cols = rep_ref.shape[:2]
    deep = held // 2
    span = deep * cols
    wide = near.shape[0]
    shift = span - (wide - LANES)
    half = half_ref[0]
    copies = [
        pltpu.make_async_copy(source, target, sems.at[at])
        for at, (source, target) in enumerate(
            (
                (rep_hbm.at[pl.ds(half * held, held)], rep_ref),
                (gain_hbm, gain_ref),
                (bias_hbm, bias_ref),
                (mask_hbm, mask_ref),
                (weight_hbm, weight_ref),
                (history_hbm, history_ref),
            )
        )
    ]
    for copy in copies:
        copy.start()
    near[pl.ds(span, wide - span), :] = jnp.zeros((wide - span, 2 * channels), BF16)
    far[pl.ds(0, shift), :] = jnp.zeros((shift, 2 * channels), BF16)
    far[pl.ds(shift + span, wide - span - shift), :] = jnp.zeros((wide - span - shift, 2 * channels), BF16)
    for copy in copies:
        copy.wait()
    for at in range(which):
        packed_ref[at * outs : (at + 1) * outs, :] = weight_ref[at]
    history = history_ref[...]
    parts = jnp.concatenate([*split_parts(history), jnp.zeros_like(history)], axis=0)
    parts = jnp.concatenate([parts, jnp.zeros_like(parts)], axis=1)
    parts = jnp.concatenate([parts, jnp.zeros_like(parts)], axis=0)
    packed_ref[which * outs :, :] = parts.astype(BF16)
    gain, bias = gain_ref[...], bias_ref[...]
    for part in range(2):
        for at in range(deep):
            block = normed_rows(rep_ref[part * deep + at].astype(F32), gain, bias)
            lanes = slice(part * channels, (part + 1) * channels)
            near[at * cols : (at + 1) * cols, lanes] = block
            far[shift + at * cols : shift + (at + 1) * cols, lanes] = block
    masks = mask_ref[...].astype(F32)
    masks = jnp.where(half == 0, masks[:held], masks[held:])
    pieces = [
        jnp.concatenate([masks[at : at + 1], masks[deep + at : deep + at + 1]], axis=0)
        for at in range(deep)
    ]
    zeros = jnp.zeros((2, wide - span), F32)
    mask_near = jnp.concatenate([jnp.concatenate([*pieces, zeros], axis=1)] * 4, axis=0)
    masks_ref[0] = mask_near
    masks_ref[1] = pltpu.roll(mask_near, shift, 1)


def history_parts(packed_ref, outs):
    start = packed_ref.shape[1] - 16
    pieces = [packed_ref[col, start:, :][:, :outs] for col in range(2)]
    return jnp.concatenate(pieces, axis=1)[:8]


def project_kernel(packed_ref, near, far, masks_ref, out_ref, proj, inverse_ref, *, span):
    wide, channels = near.shape[0], near.shape[1] // 2
    outs = channels // 2
    shift = span - (wide - LANES)
    inverse_ref[...] = format_limit / columns_of_parts(history_parts(packed_ref, outs), channels)
    even, odd = one_hot_rows(channels, 0), one_hot_rows(channels, 1)
    for which in range(4):
        here = pl.ds(which * outs, outs)
        weight = jnp.concatenate([packed_ref[0, here, :], packed_ref[1, here, :]], axis=0)
        weight = jnp.concatenate([nn(even, weight), nn(odd, weight)], axis=1).astype(BF16)
        proj[which] = nt(weight, (near if which < 2 else far)[...])
    mask_near = jnp.concatenate([masks_ref[0]] * 2, axis=0)
    mask_far = jnp.concatenate([masks_ref[1]] * 2, axis=0)
    lane = lax.broadcasted_iota(jnp.int32, (16, LANES), 1)
    first = shift + span - (wide - LANES)

    def step(at, carry):
        rows_at = pl.ds(pl.multiple_of(at * 16, 16), 16)
        left = mask_near * jax.nn.sigmoid(proj[1, rows_at, :]) * proj[0, rows_at, :]
        right = mask_far * jax.nn.sigmoid(proj[3, rows_at, :]) * proj[2, rows_at, :]
        left_max = jnp.max(jnp.abs(left), axis=1, keepdims=True)
        right_max = jnp.max(jnp.abs(right), axis=1, keepdims=True)
        inverse = inverse_ref[rows_at, :]
        left = jnp.clip(left * inverse[:, 0:1], -format_limit, format_limit)
        right = jnp.clip(right * inverse[:, 1:2], -format_limit, format_limit)
        edge = wide - LANES
        peers_at = pl.ds(at * 8, 8)

        def put(start, stop, values):
            out_ref[peers_at, :, start:stop] = values.astype(BF16).reshape(8, 2, stop - start)

        put(0, edge, left[:, :edge])
        put(edge, wide, left[:, edge:] + right[:, :LANES])
        put(wide, wide + edge - LANES, right[:, LANES:edge])
        last = right[:, edge:]
        for place, part in enumerate((*split_parts(left_max), *split_parts(right_max))):
            last = jnp.where(lane == first + place, part, last)
        put(wide + edge - LANES, wide + edge, last)
        return carry

    lax.fori_loop(0, 2 * channels // 16, step, 0)


def gate_kernel(
    mine_ref,
    rep_ref,
    packed_ref,
    gate_ref,
    weight_ref,
    gain_ref,
    bias_ref,
    affine_ref,
    gating_ref,
    mixer_ref,
    order_ref,
    columns_ref,
    scale_ref,
    near,
):
    rows, cols, channels = rep_ref.shape
    deep = rows // 4
    span = deep * cols
    outs = gate_ref.shape[0]
    gain, bias = gain_ref[...], bias_ref[...]
    blank = jnp.zeros((outs, channels), BF16)
    gate = gate_ref[...]
    wide_gate = jnp.concatenate(
        [jnp.concatenate([gate, blank], axis=1), jnp.concatenate([blank, gate], axis=1)], axis=0
    )
    near[span:, :] = jnp.zeros((near.shape[0] - span, 2 * channels), BF16)
    for half in range(2):
        for part in range(2):
            for at in range(deep):
                block = rep_ref[half * (2 * deep) + part * deep + at].astype(F32)
                near[at * cols : (at + 1) * cols, part * channels : (part + 1) * channels] = normed_rows(
                    block, gain, bias
                )
        gating_ref[half] = jax.nn.sigmoid(nt(wide_gate, near[...]))
    columns_ref[...] = columns_of(affine_ref[...], channels)
    parts = history_parts(packed_ref, outs).astype(F32)
    lane = lax.broadcasted_iota(jnp.int32, parts.shape, 1)
    parts = jnp.sum(jnp.where(lane == mine_ref[0], parts, 0.0), axis=1, keepdims=True)
    scales = (parts[0:2] + parts[2:4] + parts[4:6]) / format_limit
    scale_ref[...] = jnp.broadcast_to(scales[0:1] * scales[1:2], scale_ref.shape)
    weight = weight_ref[...]
    mixer_ref[0:outs, :] = nn(weight, one_hot_cols(channels, 0)).astype(BF16)
    mixer_ref[outs:, :] = nn(weight, one_hot_cols(channels, 1)).astype(BF16)
    count, lanes = order_ref.shape
    per_half = count // 2
    per_at = per_half // deep
    pairs = cols // rows
    step = 32
    for start in range(0, count, step):
        row = start + lax.broadcasted_iota(jnp.int32, (step, 1), 0)
        half_at = start // per_half
        deep_at = (start % per_half) // per_at
        block = (row - half_at * per_half - deep_at * per_at) >> 1
        part = row & 1
        target = (block // pairs) * LANES + (block % pairs) * rows + half_at * 2 * deep + part * deep + deep_at
        lane = lax.broadcasted_iota(jnp.int32, (step, lanes), 1)
        order_ref[start : start + step, :] = jnp.where(lane == target, 1.0, 0.0).astype(BF16)


def unpack_kernel(received_ref, left_ref, right_ref, flat, *, groups, deep, cols):
    rows, lanes = flat.shape
    block = rows // groups
    span = deep * cols
    for group in range(groups):
        piece = received_ref[group * block // 2 : (group + 1) * block // 2]
        flat[group * block : (group + 1) * block, :] = piece.reshape(block, lanes)

    def window(group, start):
        base = start // LANES * LANES
        stop = -(-(start + cols) // LANES) * LANES
        return flat[group * block : (group + 1) * block, base:stop][:, start - base : start - base + cols]

    for at in range(deep):
        place = pl.ds(at * block, block)
        left_ref[place, :] = jnp.concatenate([window(g, at * cols) for g in range(groups)], axis=1)
        right_ref[place, :] = jnp.concatenate([window(g, span + at * cols) for g in range(groups)], axis=1)
    parts = flat[:, lanes - LANES :].astype(F32)
    total = parts + pltpu.roll(parts, LANES - 1, 1) + pltpu.roll(parts, LANES - 2, 1)
    best = jnp.max(jnp.max(total.reshape(rows // 8, 8, LANES), axis=0), axis=0, keepdims=True)
    best = jnp.concatenate([*split_parts(best), jnp.zeros((13, LANES), F32)], axis=0).astype(BF16)
    right_ref[deep * block :, :] = jnp.concatenate(
        [best, jnp.zeros((16, groups * cols - LANES), BF16)], axis=1
    )


def triangle_kernel(scale_ref, left_ref, both_ref, order_ref, out_ref, moved, *, groups, deep, cols):
    count = left_ref.shape[0]
    block = count // deep
    span = deep * cols
    scale = scale_ref[0:1, 0:1]
    total = None
    best = None
    for other in range(2):
        products = nt(left_ref[...], both_ref[other, :count, :]) * scale
        turned = nn(products.astype(BF16), order_ref[other * count : (other + 1) * count, :])
        total = turned if total is None else total + turned
        parts = both_ref[other, count:, :LANES].astype(F32)
        parts = parts[0:1] + parts[1:2] + parts[2:3]
        best = parts if best is None else jnp.maximum(best, parts)
    moved[...] = total.astype(BF16)
    lane = lax.broadcasted_iota(jnp.int32, (8, LANES), 1)
    first = 2 * span % LANES
    goal = span % LANES
    best = jnp.broadcast_to(best, (8, LANES))
    tail = jnp.zeros((8, LANES), F32)
    for place, part in enumerate(split_parts(best)):
        turned = pltpu.roll(part, (goal + place - first) % LANES, 1)
        tail = jnp.where((lane == goal + place) | (lane == goal + place + 3), turned, tail)
    tail = jnp.broadcast_to(tail[0:1, goal:], (block, LANES - goal)).astype(BF16)
    for group in range(groups):
        pieces = [
            moved[at * block : (at + 1) * block, group * LANES : group * LANES + cols] for at in range(deep)
        ]
        pieces = jnp.concatenate([*pieces, tail], axis=1)
        out_ref[group * block // 2 : (group + 1) * block // 2] = pieces.reshape(block // 2, 2, -1)


def finish_kernel(
    half_ref, both_ref, gating_ref, mixer_ref, columns_ref, update_ref, amax_ref, mixed, *, deep, cols
):
    rows, wide = both_ref.shape[1:]
    channels = rows // 2
    outs = update_ref.shape[1]
    span = deep * cols
    gain, bias = columns_ref[:, 0:1], columns_ref[:, 1:2]
    mixer = mixer_ref[...]

    def per_part(values):
        total = jnp.sum(values, axis=0)
        total = total + pltpu.roll(total, 4, 0)
        total = total + pltpu.roll(total, 2, 0)
        return total * (1.0 / channels)

    for half in range(2):
        for start in range(0, wide, LANES):
            values = both_ref[half, :, start : start + LANES].astype(F32).reshape(rows // 8, 8, LANES)
            values = values - per_part(values)[None]
            spread = per_part(jnp.square(values))
            values = (values * lax.rsqrt(spread + epsilon)[None]).reshape(rows, LANES)
            tnorm = (values * gain + bias).astype(BF16)
            mixing = nn(mixer, tnorm)
            mixed[:, start : start + LANES] = (gating_ref[half, :, start : start + LANES] * mixing).astype(BF16)
        for part in range(2):
            for at in range(deep):
                place = half * 2 * deep + part * deep + at
                update_ref[place] = mixed[part * outs : (part + 1) * outs, at * cols : (at + 1) * cols]
    last = both_ref[0, :, wide - LANES :]
    row = lax.broadcasted_iota(jnp.int32, (rows, outs), 0)
    col = lax.broadcasted_iota(jnp.int32, (rows, outs), 1)
    chosen = jnp.where(row == 2 * (col + half_ref[0] * outs), 1.0, 0.0).astype(BF16)
    sums = lax.dot_general(last, chosen, (((0,), (0,)), ((), ())), preferred_element_type=F32)
    goal = span % LANES
    amax_ref[0:1, :] = sums[goal : goal + 1] + sums[goal + 1 : goal + 2] + sums[goal + 2 : goal + 3]
    amax_ref[1:2, :] = sums[goal + 3 : goal + 4] + sums[goal + 4 : goal + 5] + sums[goal + 5 : goal + 6]


VMEM = pl.BlockSpec(memory_space=pltpu.VMEM)
HBM = pl.BlockSpec(memory_space=pltpu.HBM)
SMEM = pl.BlockSpec(memory_space=pltpu.SMEM)
GRANT = pltpu.CompilerParams(vmem_limit_bytes=24 * 2**20)


def on_device(
    pair_rep,
    pair_mask,
    amax_history,
    in_gain,
    in_bias,
    proj_weight,
    gate_weight,
    out_gain,
    out_bias,
    out_weight,
):
    rows, cols, channels = pair_rep.shape[1:]
    deep = rows // 4
    span = deep * cols
    wide = lane_round(span)
    groups, ranks = lax.axis_size("gy"), lax.axis_size("gx")
    chips = ("gy", "gx")
    assert groups * ranks == channels and lax.axis_size("col") == 2
    half = lax.axis_index("col").reshape(1).astype(jnp.int32)
    rep = pair_rep[0]
    gain, bias = in_gain[None, :], in_bias[None, :]

    packed, near, far, masks = pl.pallas_call(
        prepare_kernel,
        name="prepare",
        out_shape=(
            jax.ShapeDtypeStruct((2 * channels + 16, channels), BF16),
            jax.ShapeDtypeStruct((wide, 2 * channels), BF16),
            jax.ShapeDtypeStruct((wide, 2 * channels), BF16),
            jax.ShapeDtypeStruct((2, 8, wide), F32),
        ),
        in_specs=[SMEM] + [HBM] * 6,
        out_specs=(VMEM,) * 4,
        scratch_shapes=[
            pltpu.VMEM((rows // 2, cols, channels), BF16),
            pltpu.VMEM((rows, cols), jnp.int32),
            pltpu.VMEM((4, channels // 2, channels), BF16),
            pltpu.VMEM((2, channels // 2), F32),
            pltpu.VMEM((1, channels), F32),
            pltpu.VMEM((1, channels), F32),
            pltpu.SemaphoreType.DMA((6,)),
        ],
        compiler_params=GRANT,
    )(half, *map(in_hbm, (rep, pair_mask[0], jnp.transpose(proj_weight, (1, 2, 0)), amax_history, gain, bias)))
    packed = lax.all_gather(packed, "col")
    message = pl.pallas_call(
        functools.partial(project_kernel, span=span),
        name="project",
        out_shape=jax.ShapeDtypeStruct((channels, 2, 2 * wide - LANES), BF16),
        in_specs=[VMEM] * 4,
        out_specs=VMEM,
        scratch_shapes=[
            pltpu.VMEM((4, 2 * channels, wide), F32),
            pltpu.VMEM((2 * channels, 2), F32),
        ],
        compiler_params=GRANT,
    )(packed, near, far, masks)
    received = lax.all_to_all(message, chips, split_axis=0, concat_axis=0, tiled=True)
    mine = lax.axis_index(chips).reshape(1).astype(jnp.int32)
    gating, mixer, order, columns, scale = pl.pallas_call(
        gate_kernel,
        name="gate",
        out_shape=(
            jax.ShapeDtypeStruct((2, channels, wide), F32),
            jax.ShapeDtypeStruct((channels, 2 * channels), BF16),
            jax.ShapeDtypeStruct((ranks * rows, groups * LANES), BF16),
            jax.ShapeDtypeStruct((2 * channels, 2), F32),
            jax.ShapeDtypeStruct((8, LANES), F32),
        ),
        in_specs=[SMEM] + [VMEM] * 7,
        out_specs=(VMEM,) * 5,
        scratch_shapes=[pltpu.VMEM((wide, 2 * channels), BF16)],
        compiler_params=GRANT,
        cost_estimate=pl.CostEstimate(flops=20_000_000_000, bytes_accessed=3_000_000, transcendentals=0),
    )(mine, rep, packed, gate_weight.T, out_weight.T, gain, bias, jnp.stack([out_gain, out_bias]))
    count = ranks * rows // 2
    left, right = pl.pallas_call(
        functools.partial(unpack_kernel, groups=groups, deep=deep, cols=cols),
        name="unpack",
        out_shape=(
            jax.ShapeDtypeStruct((count, groups * cols), BF16),
            jax.ShapeDtypeStruct((count + 16, groups * cols), BF16),
        ),
        in_specs=[VMEM],
        out_specs=(VMEM,) * 2,
        scratch_shapes=[pltpu.VMEM((2 * channels, 2 * wide - LANES), BF16)],
        compiler_params=GRANT,
    )(received)
    both = lax.all_gather(right, "col")
    products = pl.pallas_call(
        functools.partial(triangle_kernel, groups=groups, deep=deep, cols=cols),
        name="triangle",
        out_shape=jax.ShapeDtypeStruct((channels, 2, wide), BF16),
        in_specs=[VMEM] * 4,
        out_specs=VMEM,
        scratch_shapes=[pltpu.VMEM((count, groups * LANES), BF16)],
        compiler_params=GRANT,
    )(scale, left, both, order)
    returned = lax.all_to_all(products, chips, split_axis=0, concat_axis=0, tiled=True)
    both = lax.all_gather(returned.reshape(2 * channels, -1), "col")
    update, new_amax = pl.pallas_call(
        functools.partial(finish_kernel, deep=deep, cols=cols),
        name="finish",
        out_shape=(
            jax.ShapeDtypeStruct((rows, channels // 2, cols), BF16),
            jax.ShapeDtypeStruct((2, channels // 2), F32),
        ),
        in_specs=[SMEM] + [VMEM] * 4,
        out_specs=(VMEM,) * 2,
        scratch_shapes=[pltpu.VMEM((channels, wide), BF16)],
        compiler_params=GRANT,
    )(half, both, gating, mixer, columns)
    return (jnp.transpose(update, (0, 2, 1))[None], new_amax)


def solution(mesh):
    placed = (
        P("ga", "gx", "gy", None),
        P("ga", "gx", "gy"),
        P(None, "col"),
        P(),
        P(),
        P(None, None, "col"),
        P(None, "col"),
        P(),
        P(),
        P(None, "col"),
    )
    return jax.shard_map(
        on_device,
        mesh=mesh,
        in_specs=placed,
        out_specs=(P("ga", "gx", "gy", "col"), P("ga", "col")),
        check_vma=False,
    )
```

```python
import functools

import jax
import jax.numpy as jnp
from jax import lax
from jax.experimental import pallas as pl
from jax.experimental.pallas import tpu as pltpu
from jax.sharding import PartitionSpec as P

epsilon = 1e-05
format_limit = 448.0
LANES = 128
F32 = jnp.float32
BF16 = jnp.bfloat16


def lane_round(size):
    return -(-size // LANES) * LANES


def normed_rows(rows, gain, bias):
    average = jnp.mean(rows, axis=-1, keepdims=True)
    spread = jnp.mean(jnp.square(rows - average), axis=-1, keepdims=True)
    return ((rows - average) * lax.rsqrt(spread + epsilon) * gain + bias).astype(BF16)


def one_hot_rows(channels, parity, dtype=BF16):
    row = lax.broadcasted_iota(jnp.int32, (2 * channels, channels), 0)
    col = lax.broadcasted_iota(jnp.int32, (2 * channels, channels), 1)
    return jnp.where(row == 2 * col + parity, 1.0, 0.0).astype(dtype)


def one_hot_cols(channels, parity):
    row = lax.broadcasted_iota(jnp.int32, (channels, 2 * channels), 0)
    col = lax.broadcasted_iota(jnp.int32, (channels, 2 * channels), 1)
    return jnp.where(col == 2 * row + parity, 1.0, 0.0).astype(BF16)


def in_hbm(array):
    return pltpu.with_memory_space_constraint(array, pltpu.HBM)


def nn(left, right):
    return jnp.dot(left, right, preferred_element_type=F32)


def nt(left, right):
    return lax.dot_general(left, right, (((1,), (1,)), ((), ())), preferred_element_type=F32)


def split_parts(values):
    high = values.astype(BF16).astype(F32)
    middle = (values - high).astype(BF16).astype(F32)
    return high, middle, values - high - middle


def columns_of(rows, channels):
    parts = jnp.concatenate([*split_parts(rows), jnp.zeros_like(rows)], axis=0).astype(BF16)
    return columns_of_parts(parts, channels)


def columns_of_parts(parts, channels):
    both = (one_hot_rows(channels, 0, F32) + one_hot_rows(channels, 1, F32)).astype(BF16)
    columns = nt(both, parts)
    return columns[:, 0:2] + columns[:, 2:4] + columns[:, 4:6]


def prepare_kernel(
    half_ref,
    rep_hbm,
    mask_hbm,
    weight_hbm,
    history_hbm,
    gain_hbm,
    bias_hbm,
    packed_ref,
    near,
    far,
    masks_ref,
    rep_ref,
    mask_ref,
    weight_ref,
    history_ref,
    gain_ref,
    bias_ref,
    sems,
):
    which, outs, channels = weight_ref.shape
    held, cols = rep_ref.shape[:2]
    deep = held // 2
    span = deep * cols
    wide = near.shape[0]
    shift = span - (wide - LANES)
    half = half_ref[0]
    copies = [
        pltpu.make_async_copy(source, target, sems.at[at])
        for at, (source, target) in enumerate(
            (
                (rep_hbm.at[pl.ds(half * held, deep)], rep_ref.at[pl.ds(0, deep)]),
                (rep_hbm.at[pl.ds(half * held + deep, deep)], rep_ref.at[pl.ds(deep, deep)]),
                (gain_hbm, gain_ref),
                (bias_hbm, bias_ref),
                (mask_hbm, mask_ref),
                (weight_hbm, weight_ref),
                (history_hbm, history_ref),
            )
        )
    ]
    for copy in copies:
        copy.start()
    near[pl.ds(span, wide - span), :] = jnp.zeros((wide - span, 2 * channels), BF16)
    far[pl.ds(0, shift), :] = jnp.zeros((shift, 2 * channels), BF16)
    far[pl.ds(shift + span, wide - span - shift), :] = jnp.zeros((wide - span - shift, 2 * channels), BF16)
    for copy in copies[2:]:
        copy.wait()
    for at in range(which):
        packed_ref[at * outs : (at + 1) * outs, :] = weight_ref[at]
    history = history_ref[...]
    parts = jnp.concatenate([*split_parts(history), jnp.zeros_like(history)], axis=0)
    parts = jnp.concatenate([parts, jnp.zeros_like(parts)], axis=1)
    parts = jnp.concatenate([parts, jnp.zeros_like(parts)], axis=0)
    packed_ref[which * outs :, :] = parts.astype(BF16)
    gain, bias = gain_ref[...], bias_ref[...]
    for part in range(2):
        copies[part].wait()
        for at in range(deep):
            block = normed_rows(rep_ref[part * deep + at].astype(F32), gain, bias)
            lanes = slice(part * channels, (part + 1) * channels)
            near[at * cols : (at + 1) * cols, lanes] = block
            far[shift + at * cols : shift + (at + 1) * cols, lanes] = block
    masks = mask_ref[...].astype(F32)
    masks = jnp.where(half == 0, masks[:held], masks[held:])
    pieces = [
        jnp.concatenate([masks[at : at + 1], masks[deep + at : deep + at + 1]], axis=0)
        for at in range(deep)
    ]
    zeros = jnp.zeros((2, wide - span), F32)
    mask_near = jnp.concatenate([jnp.concatenate([*pieces, zeros], axis=1)] * 4, axis=0)
    masks_ref[0] = mask_near
    masks_ref[1] = pltpu.roll(mask_near, shift, 1)


def history_parts(packed_ref, outs):
    start = packed_ref.shape[1] - 16
    pieces = [packed_ref[col, start:, :][:, :outs] for col in range(2)]
    return jnp.concatenate(pieces, axis=1)[:8]


def project_kernel(packed_ref, near, far, masks_ref, out_hbm, proj, inverse_ref, out_ref, sems, *, span):
    wide, channels = near.shape[0], near.shape[1] // 2
    outs = channels // 2
    shift = span - (wide - LANES)
    inverse_ref[...] = format_limit / columns_of_parts(history_parts(packed_ref, outs), channels)
    even, odd = one_hot_rows(channels, 0), one_hot_rows(channels, 1)
    for which in range(4):
        here = pl.ds(which * outs, outs)
        weight = jnp.concatenate([packed_ref[0, here, :], packed_ref[1, here, :]], axis=0)
        weight = jnp.concatenate([nn(even, weight), nn(odd, weight)], axis=1).astype(BF16)
        proj[which] = nt(weight, (near if which < 2 else far)[...])
    mask_near = jnp.concatenate([masks_ref[0]] * 2, axis=0)
    mask_far = jnp.concatenate([masks_ref[1]] * 2, axis=0)
    lane = lax.broadcasted_iota(jnp.int32, (16, LANES), 1)
    first = shift + span - (wide - LANES)

    def step(at, carry):
        rows_at = pl.ds(pl.multiple_of(at * 16, 16), 16)
        left = mask_near * jax.nn.sigmoid(proj[1, rows_at, :]) * proj[0, rows_at, :]
        right = mask_far * jax.nn.sigmoid(proj[3, rows_at, :]) * proj[2, rows_at, :]
        left_max = jnp.max(jnp.abs(left), axis=1, keepdims=True)
        right_max = jnp.max(jnp.abs(right), axis=1, keepdims=True)
        inverse = inverse_ref[rows_at, :]
        left = jnp.clip(left * inverse[:, 0:1], -format_limit, format_limit)
        right = jnp.clip(right * inverse[:, 1:2], -format_limit, format_limit)
        edge = wide - LANES
        peers_at = pl.ds(at * 8, 8)

        def put(start, stop, values):
            out_ref[peers_at, :, start:stop] = values.astype(BF16).reshape(8, 2, stop - start)

        put(0, edge, left[:, :edge])
        put(edge, wide, left[:, edge:] + right[:, :LANES])
        put(wide, wide + edge - LANES, right[:, LANES:edge])
        last = right[:, edge:]
        for place, part in enumerate((*split_parts(left_max), *split_parts(right_max))):
            last = jnp.where(lane == first + place, part, last)
        put(wide + edge - LANES, wide + edge, last)
        sent(at).start()
        return carry

    def sent(at):
        peers_at = pl.ds(at * 8, 8)
        return pltpu.make_async_copy(out_ref.at[peers_at], out_hbm.at[peers_at], sems.at[at])

    def settle(at, carry):
        sent(at).wait()
        return carry

    lax.fori_loop(0, channels // 8, step, 0)
    lax.fori_loop(0, channels // 8, settle, 0)


def gate_kernel(
    mine_ref,
    rep_ref,
    packed_ref,
    gate_ref,
    weight_ref,
    gain_ref,
    bias_ref,
    affine_ref,
    gating_ref,
    mixer_ref,
    order_ref,
    columns_ref,
    scale_ref,
    near,
):
    rows, cols, channels = rep_ref.shape
    deep = rows // 4
    span = deep * cols
    outs = gate_ref.shape[0]
    gain, bias = gain_ref[...], bias_ref[...]
    blank = jnp.zeros((outs, channels), BF16)
    gate = gate_ref[...]
    wide_gate = jnp.concatenate(
        [jnp.concatenate([gate, blank], axis=1), jnp.concatenate([blank, gate], axis=1)], axis=0
    )
    near[span:, :] = jnp.zeros((near.shape[0] - span, 2 * channels), BF16)
    for half in range(2):
        for part in range(2):
            for at in range(deep):
                block = rep_ref[half * (2 * deep) + part * deep + at].astype(F32)
                near[at * cols : (at + 1) * cols, part * channels : (part + 1) * channels] = normed_rows(
                    block, gain, bias
                )
        gating_ref[half] = jax.nn.sigmoid(nt(wide_gate, near[...]))
    columns_ref[...] = columns_of(affine_ref[...], channels)
    parts = history_parts(packed_ref, outs).astype(F32)
    lane = lax.broadcasted_iota(jnp.int32, parts.shape, 1)
    parts = jnp.sum(jnp.where(lane == mine_ref[0], parts, 0.0), axis=1, keepdims=True)
    scales = (parts[0:2] + parts[2:4] + parts[4:6]) / format_limit
    scale_ref[...] = jnp.broadcast_to(scales[0:1] * scales[1:2], scale_ref.shape)
    weight = weight_ref[...]
    mixer_ref[0:outs, :] = nn(weight, one_hot_cols(channels, 0)).astype(BF16)
    mixer_ref[outs:, :] = nn(weight, one_hot_cols(channels, 1)).astype(BF16)
    count, lanes = order_ref.shape
    per_half = count // 2
    per_at = per_half // deep
    pairs = cols // rows
    step = 32
    for start in range(0, count, step):
        row = start + lax.broadcasted_iota(jnp.int32, (step, 1), 0)
        half_at = start // per_half
        deep_at = (start % per_half) // per_at
        block = (row - half_at * per_half - deep_at * per_at) >> 1
        part = row & 1
        target = (block // pairs) * LANES + (block % pairs) * rows + half_at * 2 * deep + part * deep + deep_at
        lane = lax.broadcasted_iota(jnp.int32, (step, lanes), 1)
        order_ref[start : start + step, :] = jnp.where(lane == target, 1.0, 0.0).astype(BF16)


def unpack_kernel(received_ref, left_ref, right_ref, flat, *, groups, deep, cols):
    rows, lanes = flat.shape
    block = rows // groups
    span = deep * cols
    for group in range(groups):
        piece = received_ref[group * block // 2 : (group + 1) * block // 2]
        flat[group * block : (group + 1) * block, :] = piece.reshape(block, lanes)

    def window(group, start):
        base = start // LANES * LANES
        stop = -(-(start + cols) // LANES) * LANES
        return flat[group * block : (group + 1) * block, base:stop][:, start - base : start - base + cols]

    for at in range(deep):
        place = pl.ds(at * block, block)
        left_ref[place, :] = jnp.concatenate([window(g, at * cols) for g in range(groups)], axis=1)
        right_ref[place, :] = jnp.concatenate([window(g, span + at * cols) for g in range(groups)], axis=1)
    parts = flat[:, lanes - LANES :].astype(F32)
    total = parts + pltpu.roll(parts, LANES - 1, 1) + pltpu.roll(parts, LANES - 2, 1)
    best = jnp.max(jnp.max(total.reshape(rows // 8, 8, LANES), axis=0), axis=0, keepdims=True)
    best = jnp.concatenate([*split_parts(best), jnp.zeros((13, LANES), F32)], axis=0).astype(BF16)
    right_ref[deep * block :, :] = jnp.concatenate(
        [best, jnp.zeros((16, groups * cols - LANES), BF16)], axis=1
    )


def triangle_kernel(scale_ref, left_ref, both_ref, order_ref, out_ref, moved, *, groups, deep, cols):
    count = left_ref.shape[0]
    block = count // deep
    span = deep * cols
    scale = scale_ref[0:1, 0:1]
    total = None
    best = None
    for other in range(2):
        products = nt(left_ref[...], both_ref[other, :count, :]) * scale
        turned = nn(products.astype(BF16), order_ref[other * count : (other + 1) * count, :])
        total = turned if total is None else total + turned
        parts = both_ref[other, count:, :LANES].astype(F32)
        parts = parts[0:1] + parts[1:2] + parts[2:3]
        best = parts if best is None else jnp.maximum(best, parts)
    moved[...] = total.astype(BF16)
    lane = lax.broadcasted_iota(jnp.int32, (8, LANES), 1)
    first = 2 * span % LANES
    goal = span % LANES
    best = jnp.broadcast_to(best, (8, LANES))
    tail = jnp.zeros((8, LANES), F32)
    for place, part in enumerate(split_parts(best)):
        turned = pltpu.roll(part, (goal + place - first) % LANES, 1)
        tail = jnp.where((lane == goal + place) | (lane == goal + place + 3), turned, tail)
    tail = jnp.broadcast_to(tail[0:1, goal:], (block, LANES - goal)).astype(BF16)
    for group in range(groups):
        pieces = [
            moved[at * block : (at + 1) * block, group * LANES : group * LANES + cols] for at in range(deep)
        ]
        pieces = jnp.concatenate([*pieces, tail], axis=1)
        out_ref[group * block // 2 : (group + 1) * block // 2] = pieces.reshape(block // 2, 2, -1)


def finish_kernel(
    half_ref, both_ref, gating_ref, mixer_ref, columns_ref, update_hbm, amax_ref, mixed, update_ref, sems, *, deep, cols
):
    rows, wide = both_ref.shape[1:]
    channels = rows // 2
    outs = update_ref.shape[1]
    span = deep * cols
    gain, bias = columns_ref[:, 0:1], columns_ref[:, 1:2]
    mixer = mixer_ref[...]

    def sent(at):
        place = pl.ds(at * deep, deep)
        return pltpu.make_async_copy(update_ref.at[place], update_hbm.at[place], sems.at[at])

    def per_part(values):
        total = jnp.sum(values, axis=0)
        total = total + pltpu.roll(total, 4, 0)
        total = total + pltpu.roll(total, 2, 0)
        return total * (1.0 / channels)

    for half in range(2):
        for start in range(0, wide, LANES):
            values = both_ref[half, :, start : start + LANES].astype(F32).reshape(rows // 8, 8, LANES)
            values = values - per_part(values)[None]
            spread = per_part(jnp.square(values))
            values = (values * lax.rsqrt(spread + epsilon)[None]).reshape(rows, LANES)
            tnorm = (values * gain + bias).astype(BF16)
            mixing = nn(mixer, tnorm)
            mixed[:, start : start + LANES] = (gating_ref[half, :, start : start + LANES] * mixing).astype(BF16)
        for part in range(2):
            for at in range(deep):
                place = half * 2 * deep + part * deep + at
                update_ref[place] = mixed[part * outs : (part + 1) * outs, at * cols : (at + 1) * cols]
            sent(2 * half + part).start()
    last = both_ref[0, :, wide - LANES :]
    row = lax.broadcasted_iota(jnp.int32, (rows, outs), 0)
    col = lax.broadcasted_iota(jnp.int32, (rows, outs), 1)
    chosen = jnp.where(row == 2 * (col + half_ref[0] * outs), 1.0, 0.0).astype(BF16)
    sums = lax.dot_general(last, chosen, (((0,), (0,)), ((), ())), preferred_element_type=F32)
    goal = span % LANES
    amax_ref[0:1, :] = sums[goal : goal + 1] + sums[goal + 1 : goal + 2] + sums[goal + 2 : goal + 3]
    amax_ref[1:2, :] = sums[goal + 3 : goal + 4] + sums[goal + 4 : goal + 5] + sums[goal + 5 : goal + 6]
    for at in range(4):
        sent(at).wait()


VMEM = pl.BlockSpec(memory_space=pltpu.VMEM)
HBM = pl.BlockSpec(memory_space=pltpu.HBM)
SMEM = pl.BlockSpec(memory_space=pltpu.SMEM)
GRANT = pltpu.CompilerParams(vmem_limit_bytes=24 * 2**20)


def on_device(
    pair_rep,
    pair_mask,
    amax_history,
    in_gain,
    in_bias,
    proj_weight,
    gate_weight,
    out_gain,
    out_bias,
    out_weight,
):
    rows, cols, channels = pair_rep.shape[1:]
    deep = rows // 4
    span = deep * cols
    wide = lane_round(span)
    groups, ranks = lax.axis_size("gy"), lax.axis_size("gx")
    chips = ("gy", "gx")
    assert groups * ranks == channels and lax.axis_size("col") == 2
    half = lax.axis_index("col").reshape(1).astype(jnp.int32)
    rep = pair_rep[0]
    gain, bias = in_gain[None, :], in_bias[None, :]

    packed, near, far, masks = pl.pallas_call(
        prepare_kernel,
        name="prepare",
        out_shape=(
            jax.ShapeDtypeStruct((2 * channels + 16, channels), BF16),
            jax.ShapeDtypeStruct((wide, 2 * channels), BF16),
            jax.ShapeDtypeStruct((wide, 2 * channels), BF16),
            jax.ShapeDtypeStruct((2, 8, wide), F32),
        ),
        in_specs=[SMEM] + [HBM] * 6,
        out_specs=(VMEM,) * 4,
        scratch_shapes=[
            pltpu.VMEM((rows // 2, cols, channels), BF16),
            pltpu.VMEM((rows, cols), jnp.int32),
            pltpu.VMEM((4, channels // 2, channels), BF16),
            pltpu.VMEM((2, channels // 2), F32),
            pltpu.VMEM((1, channels), F32),
            pltpu.VMEM((1, channels), F32),
            pltpu.SemaphoreType.DMA((7,)),
        ],
        compiler_params=GRANT,
    )(half, *map(in_hbm, (rep, pair_mask[0], jnp.transpose(proj_weight, (1, 2, 0)), amax_history, gain, bias)))
    packed = lax.all_gather(packed, "col")
    message = pl.pallas_call(
        functools.partial(project_kernel, span=span),
        name="project",
        out_shape=pltpu.HBM((channels, 2, 2 * wide - LANES), BF16),
        in_specs=[VMEM] * 4,
        out_specs=HBM,
        scratch_shapes=[
            pltpu.VMEM((4, 2 * channels, wide), F32),
            pltpu.VMEM((2 * channels, 2), F32),
            pltpu.VMEM((channels, 2, 2 * wide - LANES), BF16),
            pltpu.SemaphoreType.DMA((channels // 8,)),
        ],
        compiler_params=GRANT,
    )(packed, near, far, masks)
    received = lax.all_to_all(message, chips, split_axis=0, concat_axis=0, tiled=True)
    mine = lax.axis_index(chips).reshape(1).astype(jnp.int32)
    gating, mixer, order, columns, scale = pl.pallas_call(
        gate_kernel,
        name="gate",
        out_shape=(
            jax.ShapeDtypeStruct((2, channels, wide), F32),
            jax.ShapeDtypeStruct((channels, 2 * channels), BF16),
            jax.ShapeDtypeStruct((ranks * rows, groups * LANES), BF16),
            jax.ShapeDtypeStruct((2 * channels, 2), F32),
            jax.ShapeDtypeStruct((8, LANES), F32),
        ),
        in_specs=[SMEM] + [VMEM] * 7,
        out_specs=(VMEM,) * 5,
        scratch_shapes=[pltpu.VMEM((wide, 2 * channels), BF16)],
        compiler_params=GRANT,
        cost_estimate=pl.CostEstimate(flops=20_000_000_000, bytes_accessed=3_000_000, transcendentals=0),
    )(mine, rep, packed, gate_weight.T, out_weight.T, gain, bias, jnp.stack([out_gain, out_bias]))
    count = ranks * rows // 2
    left, right = pl.pallas_call(
        functools.partial(unpack_kernel, groups=groups, deep=deep, cols=cols),
        name="unpack",
        out_shape=(
            jax.ShapeDtypeStruct((count, groups * cols), BF16),
            jax.ShapeDtypeStruct((count + 16, groups * cols), BF16),
        ),
        in_specs=[VMEM],
        out_specs=(VMEM,) * 2,
        scratch_shapes=[pltpu.VMEM((2 * channels, 2 * wide - LANES), BF16)],
        compiler_params=GRANT,
    )(received)
    both = lax.all_gather(right, "col")
    products = pl.pallas_call(
        functools.partial(triangle_kernel, groups=groups, deep=deep, cols=cols),
        name="triangle",
        out_shape=jax.ShapeDtypeStruct((channels, 2, wide), BF16),
        in_specs=[VMEM] * 4,
        out_specs=VMEM,
        scratch_shapes=[pltpu.VMEM((count, groups * LANES), BF16)],
        compiler_params=GRANT,
    )(scale, left, both, order)
    returned = lax.all_to_all(products, chips, split_axis=0, concat_axis=0, tiled=True)
    both = lax.all_gather(returned.reshape(2 * channels, -1), "col")
    update, new_amax = pl.pallas_call(
        functools.partial(finish_kernel, deep=deep, cols=cols),
        name="finish",
        out_shape=(
            pltpu.HBM((rows, channels // 2, cols), BF16),
            jax.ShapeDtypeStruct((2, channels // 2), F32),
        ),
        in_specs=[SMEM] + [VMEM] * 4,
        out_specs=(HBM, VMEM),
        scratch_shapes=[
            pltpu.VMEM((channels, wide), BF16),
            pltpu.VMEM((rows, channels // 2, cols), BF16),
            pltpu.SemaphoreType.DMA((4,)),
        ],
        compiler_params=GRANT,
    )(half, both, gating, mixer, columns)
    return (jnp.transpose(update, (0, 2, 1))[None], new_amax)


def solution(mesh):
    placed = (
        P("ga", "gx", "gy", None),
        P("ga", "gx", "gy"),
        P(None, "col"),
        P(),
        P(),
        P(None, None, "col"),
        P(None, "col"),
        P(),
        P(),
        P(None, "col"),
    )
    return jax.shard_map(
        on_device,
        mesh=mesh,
        in_specs=placed,
        out_specs=(P("ga", "gx", "gy", "col"), P("ga", "col")),
        check_vma=False,
    )
```

```python
import functools

import jax
import jax.numpy as jnp
from jax import lax
from jax.experimental import pallas as pl
from jax.experimental.pallas import tpu as pltpu
from jax.sharding import PartitionSpec as P

epsilon = 1e-05
format_limit = 448.0
LANES = 128
F32 = jnp.float32
BF16 = jnp.bfloat16


def lane_round(size):
    return -(-size // LANES) * LANES


def normed_rows(rows, gain, bias):
    average = jnp.mean(rows, axis=-1, keepdims=True)
    spread = jnp.mean(jnp.square(rows - average), axis=-1, keepdims=True)
    return ((rows - average) * lax.rsqrt(spread + epsilon) * gain + bias).astype(BF16)


def one_hot_rows(channels, parity, dtype=BF16):
    row = lax.broadcasted_iota(jnp.int32, (2 * channels, channels), 0)
    col = lax.broadcasted_iota(jnp.int32, (2 * channels, channels), 1)
    return jnp.where(row == 2 * col + parity, 1.0, 0.0).astype(dtype)


def one_hot_cols(channels, parity):
    row = lax.broadcasted_iota(jnp.int32, (channels, 2 * channels), 0)
    col = lax.broadcasted_iota(jnp.int32, (channels, 2 * channels), 1)
    return jnp.where(col == 2 * row + parity, 1.0, 0.0).astype(BF16)


def in_hbm(array):
    return pltpu.with_memory_space_constraint(array, pltpu.HBM)


def nn(left, right):
    return jnp.dot(left, right, preferred_element_type=F32)


def nt(left, right):
    return lax.dot_general(left, right, (((1,), (1,)), ((), ())), preferred_element_type=F32)


def split_parts(values):
    high = values.astype(BF16).astype(F32)
    middle = (values - high).astype(BF16).astype(F32)
    return high, middle, values - high - middle


def columns_of(rows, channels):
    parts = jnp.concatenate([*split_parts(rows), jnp.zeros_like(rows)], axis=0).astype(BF16)
    return columns_of_parts(parts, channels)


def columns_of_parts(parts, channels):
    both = (one_hot_rows(channels, 0, F32) + one_hot_rows(channels, 1, F32)).astype(BF16)
    columns = nt(both, parts)
    return columns[:, 0:2] + columns[:, 2:4] + columns[:, 4:6]


def prepare_kernel(
    half_ref,
    rep_hbm,
    mask_hbm,
    weight_hbm,
    history_hbm,
    gain_hbm,
    bias_hbm,
    packed_ref,
    near,
    far,
    masks_ref,
    rep_ref,
    mask_ref,
    weight_ref,
    history_ref,
    gain_ref,
    bias_ref,
    sems,
):
    which, outs, channels = weight_ref.shape
    held, cols = rep_ref.shape[:2]
    deep = held // 2
    span = deep * cols
    wide = near.shape[0]
    shift = span - (wide - LANES)
    half = half_ref[0]
    copies = [
        pltpu.make_async_copy(source, target, sems.at[at])
        for at, (source, target) in enumerate(
            (
                (rep_hbm.at[pl.ds(half * held, deep)], rep_ref.at[pl.ds(0, deep)]),
                (rep_hbm.at[pl.ds(half * held + deep, deep)], rep_ref.at[pl.ds(deep, deep)]),
                (gain_hbm, gain_ref),
                (bias_hbm, bias_ref),
                (mask_hbm, mask_ref),
                (weight_hbm, weight_ref),
                (history_hbm, history_ref),
            )
        )
    ]
    for copy in copies:
        copy.start()
    near[pl.ds(span, wide - span), :] = jnp.zeros((wide - span, 2 * channels), BF16)
    far[pl.ds(0, shift), :] = jnp.zeros((shift, 2 * channels), BF16)
    far[pl.ds(shift + span, wide - span - shift), :] = jnp.zeros((wide - span - shift, 2 * channels), BF16)
    for copy in copies[2:]:
        copy.wait()
    for at in range(which):
        packed_ref[at * outs : (at + 1) * outs, :] = weight_ref[at]
    history = history_ref[...]
    parts = jnp.concatenate([*split_parts(history), jnp.zeros_like(history)], axis=0)
    parts = jnp.concatenate([parts, jnp.zeros_like(parts)], axis=1)
    parts = jnp.concatenate([parts, jnp.zeros_like(parts)], axis=0)
    packed_ref[which * outs :, :] = parts.astype(BF16)
    gain, bias = gain_ref[...], bias_ref[...]
    for part in range(2):
        copies[part].wait()
        for at in range(deep):
            block = normed_rows(rep_ref[part * deep + at].astype(F32), gain, bias)
            lanes = slice(part * channels, (part + 1) * channels)
            near[at * cols : (at + 1) * cols, lanes] = block
            far[shift + at * cols : shift + (at + 1) * cols, lanes] = block
    masks = mask_ref[...].astype(F32)
    masks = jnp.where(half == 0, masks[:held], masks[held:])
    pieces = [
        jnp.concatenate([masks[at : at + 1], masks[deep + at : deep + at + 1]], axis=0)
        for at in range(deep)
    ]
    zeros = jnp.zeros((2, wide - span), F32)
    mask_near = jnp.concatenate([jnp.concatenate([*pieces, zeros], axis=1)] * 4, axis=0)
    masks_ref[0] = mask_near
    masks_ref[1] = pltpu.roll(mask_near, shift, 1)


def history_parts(packed_ref, outs):
    start = packed_ref.shape[1] - 16
    pieces = [packed_ref[col, start:, :][:, :outs] for col in range(2)]
    return jnp.concatenate(pieces, axis=1)[:8]


def project_kernel(packed_ref, near, far, masks_ref, out_hbm, proj, inverse_ref, out_ref, sems, *, span):
    wide, channels = near.shape[0], near.shape[1] // 2
    outs = channels // 2
    shift = span - (wide - LANES)
    inverse_ref[...] = format_limit / columns_of_parts(history_parts(packed_ref, outs), channels)
    even, odd = one_hot_rows(channels, 0), one_hot_rows(channels, 1)
    weight = jnp.concatenate(
        [
            jnp.concatenate([packed_ref[0, at * outs : (at + 1) * outs], packed_ref[1, at * outs : (at + 1) * outs]], axis=0)
            for at in range(4)
        ],
        axis=1,
    )
    evens, odds = nn(even, weight).astype(BF16), nn(odd, weight).astype(BF16)
    for side in range(2):
        both = [
            jnp.concatenate([held[:, at * channels : (at + 1) * channels] for held in (evens, odds)], axis=1)
            for at in (2 * side, 2 * side + 1)
        ]
        values = nt(jnp.concatenate(both, axis=0), (near if side == 0 else far)[...])
        proj[2 * side : 2 * side + 2] = values.reshape(2, 2 * channels, wide)
    mask_near = jnp.concatenate([masks_ref[0]] * 2, axis=0)
    mask_far = jnp.concatenate([masks_ref[1]] * 2, axis=0)
    lane = lax.broadcasted_iota(jnp.int32, (16, LANES), 1)
    first = shift + span - (wide - LANES)

    def step(at, carry):
        rows_at = pl.ds(pl.multiple_of(at * 16, 16), 16)
        left = mask_near * jax.nn.sigmoid(proj[1, rows_at, :]) * proj[0, rows_at, :]
        right = mask_far * jax.nn.sigmoid(proj[3, rows_at, :]) * proj[2, rows_at, :]
        left_max = jnp.max(jnp.abs(left), axis=1, keepdims=True)
        right_max = jnp.max(jnp.abs(right), axis=1, keepdims=True)
        inverse = inverse_ref[rows_at, :]
        left = jnp.clip(left * inverse[:, 0:1], -format_limit, format_limit)
        right = jnp.clip(right * inverse[:, 1:2], -format_limit, format_limit)
        edge = wide - LANES
        peers_at = pl.ds(at * 8, 8)

        def put(start, stop, values):
            out_ref[peers_at, :, start:stop] = values.astype(BF16).reshape(8, 2, stop - start)

        put(0, edge, left[:, :edge])
        put(edge, wide, left[:, edge:] + right[:, :LANES])
        put(wide, wide + edge - LANES, right[:, LANES:edge])
        last = right[:, edge:]
        for place, part in enumerate((*split_parts(left_max), *split_parts(right_max))):
            last = jnp.where(lane == first + place, part, last)
        put(wide + edge - LANES, wide + edge, last)
        sent(at).start()
        return carry

    def sent(at):
        peers_at = pl.ds(at * 8, 8)
        return pltpu.make_async_copy(out_ref.at[peers_at], out_hbm.at[peers_at], sems.at[at])

    def settle(at, carry):
        sent(at).wait()
        return carry

    lax.fori_loop(0, channels // 8, step, 0, unroll=8)
    lax.fori_loop(0, channels // 8, settle, 0)


def gate_kernel(
    mine_ref,
    rep_ref,
    packed_ref,
    gate_ref,
    weight_ref,
    gain_ref,
    bias_ref,
    affine_ref,
    gating_ref,
    mixer_ref,
    order_ref,
    columns_ref,
    scale_ref,
    near,
):
    rows, cols, channels = rep_ref.shape
    deep = rows // 4
    span = deep * cols
    outs = gate_ref.shape[0]
    gain, bias = gain_ref[...], bias_ref[...]
    blank = jnp.zeros((outs, channels), BF16)
    gate = gate_ref[...]
    wide_gate = jnp.concatenate(
        [jnp.concatenate([gate, blank], axis=1), jnp.concatenate([blank, gate], axis=1)], axis=0
    )
    near[span:, :] = jnp.zeros((near.shape[0] - span, 2 * channels), BF16)
    for half in range(2):
        for part in range(2):
            for at in range(deep):
                block = rep_ref[half * (2 * deep) + part * deep + at].astype(F32)
                near[at * cols : (at + 1) * cols, part * channels : (part + 1) * channels] = normed_rows(
                    block, gain, bias
                )
        gating_ref[half] = jax.nn.sigmoid(nt(wide_gate, near[...]))
    columns_ref[...] = columns_of(affine_ref[...], channels)
    parts = history_parts(packed_ref, outs).astype(F32)
    lane = lax.broadcasted_iota(jnp.int32, parts.shape, 1)
    parts = jnp.sum(jnp.where(lane == mine_ref[0], parts, 0.0), axis=1, keepdims=True)
    scales = (parts[0:2] + parts[2:4] + parts[4:6]) / format_limit
    scale_ref[...] = jnp.broadcast_to(scales[0:1] * scales[1:2], scale_ref.shape)
    weight = weight_ref[...]
    mixer_ref[0:outs, :] = nn(weight, one_hot_cols(channels, 0)).astype(BF16)
    mixer_ref[outs:, :] = nn(weight, one_hot_cols(channels, 1)).astype(BF16)
    count, lanes = order_ref.shape
    per_half = count // 2
    per_at = per_half // deep
    pairs = cols // rows
    step = 32
    for start in range(0, count, step):
        row = start + lax.broadcasted_iota(jnp.int32, (step, 1), 0)
        half_at = start // per_half
        deep_at = (start % per_half) // per_at
        block = (row - half_at * per_half - deep_at * per_at) >> 1
        part = row & 1
        target = (block // pairs) * LANES + (block % pairs) * rows + half_at * 2 * deep + part * deep + deep_at
        lane = lax.broadcasted_iota(jnp.int32, (step, lanes), 1)
        order_ref[start : start + step, :] = jnp.where(lane == target, 1.0, 0.0).astype(BF16)


def unpack_kernel(received_ref, left_ref, right_ref, flat, *, groups, deep, cols):
    rows, lanes = flat.shape
    block = rows // groups
    span = deep * cols
    for group in range(groups):
        piece = received_ref[group * block // 2 : (group + 1) * block // 2]
        flat[group * block : (group + 1) * block, :] = piece.reshape(block, lanes)

    def window(group, start):
        base = start // LANES * LANES
        stop = -(-(start + cols) // LANES) * LANES
        return flat[group * block : (group + 1) * block, base:stop][:, start - base : start - base + cols]

    for at in range(deep):
        place = pl.ds(at * block, block)
        left_ref[place, :] = jnp.concatenate([window(g, at * cols) for g in range(groups)], axis=1)
        right_ref[place, :] = jnp.concatenate([window(g, span + at * cols) for g in range(groups)], axis=1)
    parts = flat[:, lanes - LANES :].astype(F32)
    total = parts + pltpu.roll(parts, LANES - 1, 1) + pltpu.roll(parts, LANES - 2, 1)
    best = jnp.max(jnp.max(total.reshape(rows // 8, 8, LANES), axis=0), axis=0, keepdims=True)
    best = jnp.concatenate([*split_parts(best), jnp.zeros((13, LANES), F32)], axis=0).astype(BF16)
    right_ref[deep * block :, :] = jnp.concatenate(
        [best, jnp.zeros((16, groups * cols - LANES), BF16)], axis=1
    )


def triangle_kernel(scale_ref, left_ref, both_ref, order_ref, out_ref, moved, *, groups, deep, cols):
    count = left_ref.shape[0]
    block = count // deep
    span = deep * cols
    scale = scale_ref[0:1, 0:1]
    total = None
    best = None
    for other in range(2):
        products = nt(left_ref[...], both_ref[other, :count, :]) * scale
        turned = nn(products.astype(BF16), order_ref[other * count : (other + 1) * count, :])
        total = turned if total is None else total + turned
        parts = both_ref[other, count:, :LANES].astype(F32)
        parts = parts[0:1] + parts[1:2] + parts[2:3]
        best = parts if best is None else jnp.maximum(best, parts)
    moved[...] = total.astype(BF16)
    lane = lax.broadcasted_iota(jnp.int32, (8, LANES), 1)
    first = 2 * span % LANES
    goal = span % LANES
    best = jnp.broadcast_to(best, (8, LANES))
    tail = jnp.zeros((8, LANES), F32)
    for place, part in enumerate(split_parts(best)):
        turned = pltpu.roll(part, (goal + place - first) % LANES, 1)
        tail = jnp.where((lane == goal + place) | (lane == goal + place + 3), turned, tail)
    tail = jnp.broadcast_to(tail[0:1, goal:], (block, LANES - goal)).astype(BF16)
    for group in range(groups):
        pieces = [
            moved[at * block : (at + 1) * block, group * LANES : group * LANES + cols] for at in range(deep)
        ]
        pieces = jnp.concatenate([*pieces, tail], axis=1)
        out_ref[group * block // 2 : (group + 1) * block // 2] = pieces.reshape(block // 2, 2, -1)


def finish_kernel(
    half_ref, both_ref, gating_ref, mixer_ref, columns_ref, update_ref, amax_ref, mixed, *, deep, cols
):
    rows, wide = both_ref.shape[1:]
    channels = rows // 2
    outs = update_ref.shape[1]
    span = deep * cols
    gain, bias = columns_ref[:, 0:1], columns_ref[:, 1:2]
    mixer = mixer_ref[...]

    def per_part(values):
        total = jnp.sum(values, axis=0)
        total = total + pltpu.roll(total, 4, 0)
        total = total + pltpu.roll(total, 2, 0)
        return total * (1.0 / channels)

    for half in range(2):
        for start in range(0, wide, LANES):
            values = both_ref[half, :, start : start + LANES].astype(F32).reshape(rows // 8, 8, LANES)
            values = values - per_part(values)[None]
            spread = per_part(jnp.square(values))
            values = (values * lax.rsqrt(spread + epsilon)[None]).reshape(rows, LANES)
            tnorm = (values * gain + bias).astype(BF16)
            mixing = nn(mixer, tnorm)
            mixed[:, start : start + LANES] = (gating_ref[half, :, start : start + LANES] * mixing).astype(BF16)
        for part in range(2):
            for at in range(deep):
                place = half * 2 * deep + part * deep + at
                update_ref[place] = mixed[part * outs : (part + 1) * outs, at * cols : (at + 1) * cols]
    last = both_ref[0, :, wide - LANES :]
    row = lax.broadcasted_iota(jnp.int32, (rows, outs), 0)
    col = lax.broadcasted_iota(jnp.int32, (rows, outs), 1)
    chosen = jnp.where(row == 2 * (col + half_ref[0] * outs), 1.0, 0.0).astype(BF16)
    sums = lax.dot_general(last, chosen, (((0,), (0,)), ((), ())), preferred_element_type=F32)
    goal = span % LANES
    amax_ref[0:1, :] = sums[goal : goal + 1] + sums[goal + 1 : goal + 2] + sums[goal + 2 : goal + 3]
    amax_ref[1:2, :] = sums[goal + 3 : goal + 4] + sums[goal + 4 : goal + 5] + sums[goal + 5 : goal + 6]


VMEM = pl.BlockSpec(memory_space=pltpu.VMEM)
HBM = pl.BlockSpec(memory_space=pltpu.HBM)
SMEM = pl.BlockSpec(memory_space=pltpu.SMEM)
GRANT = pltpu.CompilerParams(vmem_limit_bytes=24 * 2**20)


def on_device(
    pair_rep,
    pair_mask,
    amax_history,
    in_gain,
    in_bias,
    proj_weight,
    gate_weight,
    out_gain,
    out_bias,
    out_weight,
):
    rows, cols, channels = pair_rep.shape[1:]
    deep = rows // 4
    span = deep * cols
    wide = lane_round(span)
    groups, ranks = lax.axis_size("gy"), lax.axis_size("gx")
    chips = ("gy", "gx")
    assert groups * ranks == channels and lax.axis_size("col") == 2
    half = lax.axis_index("col").reshape(1).astype(jnp.int32)
    rep = pair_rep[0]
    gain, bias = in_gain[None, :], in_bias[None, :]

    packed, near, far, masks = pl.pallas_call(
        prepare_kernel,
        name="prepare",
        out_shape=(
            jax.ShapeDtypeStruct((2 * channels + 16, channels), BF16),
            jax.ShapeDtypeStruct((wide, 2 * channels), BF16),
            jax.ShapeDtypeStruct((wide, 2 * channels), BF16),
            jax.ShapeDtypeStruct((2, 8, wide), F32),
        ),
        in_specs=[SMEM] + [HBM] * 6,
        out_specs=(VMEM,) * 4,
        scratch_shapes=[
            pltpu.VMEM((rows // 2, cols, channels), BF16),
            pltpu.VMEM((rows, cols), jnp.int32),
            pltpu.VMEM((4, channels // 2, channels), BF16),
            pltpu.VMEM((2, channels // 2), F32),
            pltpu.VMEM((1, channels), F32),
            pltpu.VMEM((1, channels), F32),
            pltpu.SemaphoreType.DMA((7,)),
        ],
        compiler_params=GRANT,
    )(half, *map(in_hbm, (rep, pair_mask[0], jnp.transpose(proj_weight, (1, 2, 0)), amax_history, gain, bias)))
    packed = lax.all_gather(packed, "col")
    message = pl.pallas_call(
        functools.partial(project_kernel, span=span),
        name="project",
        out_shape=pltpu.HBM((channels, 2, 2 * wide - LANES), BF16),
        in_specs=[VMEM] * 4,
        out_specs=HBM,
        scratch_shapes=[
            pltpu.VMEM((4, 2 * channels, wide), F32),
            pltpu.VMEM((2 * channels, 2), F32),
            pltpu.VMEM((channels, 2, 2 * wide - LANES), BF16),
            pltpu.SemaphoreType.DMA((channels // 8,)),
        ],
        compiler_params=GRANT,
    )(packed, near, far, masks)
    received = lax.all_to_all(message, chips, split_axis=0, concat_axis=0, tiled=True)
    mine = lax.axis_index(chips).reshape(1).astype(jnp.int32)
    gating, mixer, order, columns, scale = pl.pallas_call(
        gate_kernel,
        name="gate",
        out_shape=(
            jax.ShapeDtypeStruct((2, channels, wide), F32),
            jax.ShapeDtypeStruct((channels, 2 * channels), BF16),
            jax.ShapeDtypeStruct((ranks * rows, groups * LANES), BF16),
            jax.ShapeDtypeStruct((2 * channels, 2), F32),
            jax.ShapeDtypeStruct((8, LANES), F32),
        ),
        in_specs=[SMEM] + [VMEM] * 7,
        out_specs=(VMEM,) * 5,
        scratch_shapes=[pltpu.VMEM((wide, 2 * channels), BF16)],
        compiler_params=GRANT,
        cost_estimate=pl.CostEstimate(flops=20_000_000_000, bytes_accessed=3_000_000, transcendentals=0),
    )(mine, rep, packed, gate_weight.T, out_weight.T, gain, bias, jnp.stack([out_gain, out_bias]))
    count = ranks * rows // 2
    left, right = pl.pallas_call(
        functools.partial(unpack_kernel, groups=groups, deep=deep, cols=cols),
        name="unpack",
        out_shape=(
            jax.ShapeDtypeStruct((count, groups * cols), BF16),
            jax.ShapeDtypeStruct((count + 16, groups * cols), BF16),
        ),
        in_specs=[VMEM],
        out_specs=(VMEM,) * 2,
        scratch_shapes=[pltpu.VMEM((2 * channels, 2 * wide - LANES), BF16)],
        compiler_params=GRANT,
    )(received)
    both = lax.all_gather(right, "col")
    products = pl.pallas_call(
        functools.partial(triangle_kernel, groups=groups, deep=deep, cols=cols),
        name="triangle",
        out_shape=jax.ShapeDtypeStruct((channels, 2, wide), BF16),
        in_specs=[VMEM] * 4,
        out_specs=VMEM,
        scratch_shapes=[pltpu.VMEM((count, groups * LANES), BF16)],
        compiler_params=GRANT,
    )(scale, left, both, order)
    returned = lax.all_to_all(products, chips, split_axis=0, concat_axis=0, tiled=True)
    both = lax.all_gather(returned.reshape(2 * channels, -1), "col")
    update, new_amax = pl.pallas_call(
        functools.partial(finish_kernel, deep=deep, cols=cols),
        name="finish",
        out_shape=(
            jax.ShapeDtypeStruct((rows, channels // 2, cols), BF16),
            jax.ShapeDtypeStruct((2, channels // 2), F32),
        ),
        in_specs=[SMEM] + [VMEM] * 4,
        out_specs=(VMEM,) * 2,
        scratch_shapes=[pltpu.VMEM((channels, wide), BF16)],
        compiler_params=GRANT,
    )(half, both, gating, mixer, columns)
    return (jnp.transpose(update, (0, 2, 1))[None], new_amax)


def solution(mesh):
    placed = (
        P("ga", "gx", "gy", None),
        P("ga", "gx", "gy"),
        P(None, "col"),
        P(),
        P(),
        P(None, None, "col"),
        P(None, "col"),
        P(),
        P(),
        P(None, "col"),
    )
    return jax.shard_map(
        on_device,
        mesh=mesh,
        in_specs=placed,
        out_specs=(P("ga", "gx", "gy", "col"), P("ga", "col")),
        check_vma=False,
    )
```

```python
import functools

import jax
import jax.numpy as jnp
from jax import lax
from jax.experimental import pallas as pl
from jax.experimental.pallas import tpu as pltpu
from jax.sharding import PartitionSpec as P

epsilon = 1e-05
format_limit = 448.0
LANES = 128
F32 = jnp.float32
BF16 = jnp.bfloat16


def lane_round(size):
    return -(-size // LANES) * LANES


def normed_rows(rows, gain, bias):
    average = jnp.mean(rows, axis=-1, keepdims=True)
    spread = jnp.mean(jnp.square(rows - average), axis=-1, keepdims=True)
    return ((rows - average) * lax.rsqrt(spread + epsilon) * gain + bias).astype(BF16)


def one_hot_rows(channels, parity, dtype=BF16):
    row = lax.broadcasted_iota(jnp.int32, (2 * channels, channels), 0)
    col = lax.broadcasted_iota(jnp.int32, (2 * channels, channels), 1)
    return jnp.where(row == 2 * col + parity, 1.0, 0.0).astype(dtype)


def one_hot_cols(channels, parity):
    row = lax.broadcasted_iota(jnp.int32, (channels, 2 * channels), 0)
    col = lax.broadcasted_iota(jnp.int32, (channels, 2 * channels), 1)
    return jnp.where(col == 2 * row + parity, 1.0, 0.0).astype(BF16)


def in_hbm(array):
    return pltpu.with_memory_space_constraint(array, pltpu.HBM)


def nn(left, right):
    return jnp.dot(left, right, preferred_element_type=F32)


def nt(left, right):
    return lax.dot_general(left, right, (((1,), (1,)), ((), ())), preferred_element_type=F32)


def split_parts(values):
    high = values.astype(BF16).astype(F32)
    middle = (values - high).astype(BF16).astype(F32)
    return high, middle, values - high - middle


def columns_of(rows, channels):
    parts = jnp.concatenate([*split_parts(rows), jnp.zeros_like(rows)], axis=0).astype(BF16)
    return columns_of_parts(parts, channels)


def columns_of_parts(parts, channels):
    both = (one_hot_rows(channels, 0, F32) + one_hot_rows(channels, 1, F32)).astype(BF16)
    columns = nt(both, parts)
    return columns[:, 0:2] + columns[:, 2:4] + columns[:, 4:6]


def prepare_kernel(
    half_ref,
    rep_hbm,
    mask_hbm,
    weight_hbm,
    history_hbm,
    gain_hbm,
    bias_hbm,
    packed_ref,
    near,
    far,
    masks_ref,
    rep_ref,
    mask_ref,
    weight_ref,
    history_ref,
    gain_ref,
    bias_ref,
    sems,
):
    which, outs, channels = weight_ref.shape
    held, cols = rep_ref.shape[:2]
    deep = held // 2
    span = deep * cols
    wide = near.shape[0]
    shift = span - (wide - LANES)
    half = half_ref[0]
    copies = [
        pltpu.make_async_copy(source, target, sems.at[at])
        for at, (source, target) in enumerate(
            (
                (rep_hbm.at[pl.ds(half * held, deep)], rep_ref.at[pl.ds(0, deep)]),
                (rep_hbm.at[pl.ds(half * held + deep, deep)], rep_ref.at[pl.ds(deep, deep)]),
                (gain_hbm, gain_ref),
                (bias_hbm, bias_ref),
                (mask_hbm, mask_ref),
                (weight_hbm, weight_ref),
                (history_hbm, history_ref),
            )
        )
    ]
    for copy in copies:
        copy.start()
    near[pl.ds(span, wide - span), :] = jnp.zeros((wide - span, 2 * channels), BF16)
    far[pl.ds(0, shift), :] = jnp.zeros((shift, 2 * channels), BF16)
    far[pl.ds(shift + span, wide - span - shift), :] = jnp.zeros((wide - span - shift, 2 * channels), BF16)
    for copy in copies[2:]:
        copy.wait()
    for at in range(which):
        packed_ref[at * outs : (at + 1) * outs, :] = weight_ref[at]
    history = history_ref[...]
    parts = jnp.concatenate([*split_parts(history), jnp.zeros_like(history)], axis=0)
    parts = jnp.concatenate([parts, jnp.zeros_like(parts)], axis=1)
    parts = jnp.concatenate([parts, jnp.zeros_like(parts)], axis=0)
    packed_ref[which * outs :, :] = parts.astype(BF16)
    gain, bias = gain_ref[...], bias_ref[...]
    for part in range(2):
        copies[part].wait()
        block = rep_ref[part * deep : (part + 1) * deep].reshape(span, channels)
        block = normed_rows(block.astype(F32), gain, bias)
        lanes = slice(part * channels, (part + 1) * channels)
        near[0:span, lanes] = block
        far[shift : shift + span, lanes] = block
    masks = mask_ref[...].astype(F32)
    masks = jnp.where(half == 0, masks[:held], masks[held:])
    pieces = [
        jnp.concatenate([masks[at : at + 1], masks[deep + at : deep + at + 1]], axis=0)
        for at in range(deep)
    ]
    zeros = jnp.zeros((2, wide - span), F32)
    mask_near = jnp.concatenate([jnp.concatenate([*pieces, zeros], axis=1)] * 4, axis=0)
    masks_ref[0] = mask_near
    masks_ref[1] = pltpu.roll(mask_near, shift, 1)


def history_parts(packed_ref, outs):
    start = packed_ref.shape[1] - 16
    pieces = [packed_ref[col, start:, :][:, :outs] for col in range(2)]
    return jnp.concatenate(pieces, axis=1)[:8]


def project_kernel(packed_ref, near, far, masks_ref, out_hbm, proj, inverse_ref, out_ref, sems, *, span):
    wide, channels = near.shape[0], near.shape[1] // 2
    outs = channels // 2
    shift = span - (wide - LANES)
    inverse_ref[...] = format_limit / columns_of_parts(history_parts(packed_ref, outs), channels)
    even, odd = one_hot_rows(channels, 0), one_hot_rows(channels, 1)
    weight = jnp.concatenate(
        [
            jnp.concatenate([packed_ref[0, at * outs : (at + 1) * outs], packed_ref[1, at * outs : (at + 1) * outs]], axis=0)
            for at in range(4)
        ],
        axis=1,
    )
    evens, odds = nn(even, weight).astype(BF16), nn(odd, weight).astype(BF16)
    for side in range(2):
        both = [
            jnp.concatenate([held[:, at * channels : (at + 1) * channels] for held in (evens, odds)], axis=1)
            for at in (2 * side, 2 * side + 1)
        ]
        values = nt(jnp.concatenate(both, axis=0), (near if side == 0 else far)[...])
        proj[2 * side : 2 * side + 2] = values.reshape(2, 2 * channels, wide)
    mask_near = jnp.concatenate([masks_ref[0]] * 2, axis=0)
    mask_far = jnp.concatenate([masks_ref[1]] * 2, axis=0)
    lane = lax.broadcasted_iota(jnp.int32, (16, LANES), 1)
    first = shift + span - (wide - LANES)

    def step(at, carry):
        rows_at = pl.ds(pl.multiple_of(at * 16, 16), 16)
        left = mask_near * jax.nn.sigmoid(proj[1, rows_at, :]) * proj[0, rows_at, :]
        right = mask_far * jax.nn.sigmoid(proj[3, rows_at, :]) * proj[2, rows_at, :]
        left_max = jnp.max(jnp.abs(left), axis=1, keepdims=True)
        right_max = jnp.max(jnp.abs(right), axis=1, keepdims=True)
        inverse = inverse_ref[rows_at, :]
        left = jnp.clip(left * inverse[:, 0:1], -format_limit, format_limit)
        right = jnp.clip(right * inverse[:, 1:2], -format_limit, format_limit)
        edge = wide - LANES
        peers_at = pl.ds(at * 8, 8)

        def put(start, stop, values):
            out_ref[peers_at, :, start:stop] = values.astype(BF16).reshape(8, 2, stop - start)

        put(0, edge, left[:, :edge])
        put(edge, wide, left[:, edge:] + right[:, :LANES])
        put(wide, wide + edge - LANES, right[:, LANES:edge])
        last = right[:, edge:]
        for place, part in enumerate((*split_parts(left_max), *split_parts(right_max))):
            last = jnp.where(lane == first + place, part, last)
        put(wide + edge - LANES, wide + edge, last)
        sent(at).start()
        return carry

    def sent(at):
        peers_at = pl.ds(at * 8, 8)
        return pltpu.make_async_copy(out_ref.at[peers_at], out_hbm.at[peers_at], sems.at[at])

    def settle(at, carry):
        sent(at).wait()
        return carry

    lax.fori_loop(0, channels // 8, step, 0, unroll=8)
    lax.fori_loop(0, channels // 8, settle, 0)


def gate_kernel(
    mine_ref,
    rep_ref,
    packed_ref,
    gate_ref,
    weight_ref,
    gain_ref,
    bias_ref,
    affine_ref,
    gating_ref,
    mixer_ref,
    order_ref,
    columns_ref,
    scale_ref,
    near,
):
    rows, cols, channels = rep_ref.shape
    deep = rows // 4
    span = deep * cols
    outs = gate_ref.shape[0]
    gain, bias = gain_ref[...], bias_ref[...]
    blank = jnp.zeros((outs, channels), BF16)
    gate = gate_ref[...]
    wide_gate = jnp.concatenate(
        [jnp.concatenate([gate, blank], axis=1), jnp.concatenate([blank, gate], axis=1)], axis=0
    )
    near[span:, :] = jnp.zeros((near.shape[0] - span, 2 * channels), BF16)
    for half in range(2):
        for part in range(2):
            start = half * (2 * deep) + part * deep
            block = rep_ref[start : start + deep].reshape(span, channels).astype(F32)
            near[0:span, part * channels : (part + 1) * channels] = normed_rows(block, gain, bias)
        gating_ref[half] = jax.nn.sigmoid(nt(wide_gate, near[...]))
    columns_ref[...] = columns_of(affine_ref[...], channels)
    parts = history_parts(packed_ref, outs).astype(F32)
    lane = lax.broadcasted_iota(jnp.int32, parts.shape, 1)
    parts = jnp.sum(jnp.where(lane == mine_ref[0], parts, 0.0), axis=1, keepdims=True)
    scales = (parts[0:2] + parts[2:4] + parts[4:6]) / format_limit
    scale_ref[...] = jnp.broadcast_to(scales[0:1] * scales[1:2], scale_ref.shape)
    weight = weight_ref[...]
    mixer_ref[0:outs, :] = nn(weight, one_hot_cols(channels, 0)).astype(BF16)
    mixer_ref[outs:, :] = nn(weight, one_hot_cols(channels, 1)).astype(BF16)
    count, lanes = order_ref.shape
    per_half = count // 2
    per_at = per_half // deep
    pairs = cols // rows
    step = 32
    for start in range(0, count, step):
        row = start + lax.broadcasted_iota(jnp.int32, (step, 1), 0)
        half_at = start // per_half
        deep_at = (start % per_half) // per_at
        block = (row - half_at * per_half - deep_at * per_at) >> 1
        part = row & 1
        target = (block // pairs) * LANES + (block % pairs) * rows + half_at * 2 * deep + part * deep + deep_at
        lane = lax.broadcasted_iota(jnp.int32, (step, lanes), 1)
        order_ref[start : start + step, :] = jnp.where(lane == target, 1.0, 0.0).astype(BF16)


def unpack_kernel(received_ref, left_ref, right_ref, flat, *, groups, deep, cols):
    rows, lanes = flat.shape
    block = rows // groups
    span = deep * cols
    for group in range(groups):
        piece = received_ref[group * block // 2 : (group + 1) * block // 2]
        flat[group * block : (group + 1) * block, :] = piece.reshape(block, lanes)

    def window(group, start):
        base = start // LANES * LANES
        stop = -(-(start + cols) // LANES) * LANES
        return flat[group * block : (group + 1) * block, base:stop][:, start - base : start - base + cols]

    for at in range(deep):
        place = pl.ds(at * block, block)
        left_ref[place, :] = jnp.concatenate([window(g, at * cols) for g in range(groups)], axis=1)
        right_ref[place, :] = jnp.concatenate([window(g, span + at * cols) for g in range(groups)], axis=1)
    parts = flat[:, lanes - LANES :].astype(F32)
    total = parts + pltpu.roll(parts, LANES - 1, 1) + pltpu.roll(parts, LANES - 2, 1)
    best = jnp.max(jnp.max(total.reshape(rows // 8, 8, LANES), axis=0), axis=0, keepdims=True)
    best = jnp.concatenate([*split_parts(best), jnp.zeros((13, LANES), F32)], axis=0).astype(BF16)
    right_ref[deep * block :, :] = jnp.concatenate(
        [best, jnp.zeros((16, groups * cols - LANES), BF16)], axis=1
    )


def triangle_kernel(scale_ref, left_ref, both_ref, order_ref, out_ref, moved, *, groups, deep, cols):
    count = left_ref.shape[0]
    block = count // deep
    span = deep * cols
    scale = scale_ref[0:1, 0:1]
    best = None
    for other in range(2):
        parts = both_ref[other, count:, :LANES].astype(F32)
        parts = parts[0:1] + parts[1:2] + parts[2:3]
        best = parts if best is None else jnp.maximum(best, parts)
    right = jnp.concatenate([both_ref[other, :count, :] for other in range(2)], axis=0)
    products = nt(left_ref[...], right) * scale
    moved[...] = nn(products.astype(BF16), order_ref[...]).astype(BF16)
    lane = lax.broadcasted_iota(jnp.int32, (8, LANES), 1)
    first = 2 * span % LANES
    goal = span % LANES
    best = jnp.broadcast_to(best, (8, LANES))
    tail = jnp.zeros((8, LANES), F32)
    for place, part in enumerate(split_parts(best)):
        turned = pltpu.roll(part, (goal + place - first) % LANES, 1)
        tail = jnp.where((lane == goal + place) | (lane == goal + place + 3), turned, tail)
    tail = jnp.broadcast_to(tail[0:1, goal:], (block, LANES - goal)).astype(BF16)
    for group in range(groups):
        pieces = [
            moved[at * block : (at + 1) * block, group * LANES : group * LANES + cols] for at in range(deep)
        ]
        pieces = jnp.concatenate([*pieces, tail], axis=1)
        out_ref[group * block // 2 : (group + 1) * block // 2] = pieces.reshape(block // 2, 2, -1)


def finish_kernel(
    half_ref, both_ref, gating_ref, mixer_ref, columns_ref, update_ref, amax_ref, mixed, *, deep, cols
):
    rows, wide = both_ref.shape[1:]
    channels = rows // 2
    outs = update_ref.shape[1]
    span = deep * cols
    gain, bias = columns_ref[:, 0:1], columns_ref[:, 1:2]
    mixer = mixer_ref[...]

    def per_part(values):
        total = jnp.sum(values, axis=0)
        total = total + pltpu.roll(total, 4, 0)
        total = total + pltpu.roll(total, 2, 0)
        return total * (1.0 / channels)

    for half in range(2):
        for start in range(0, wide, LANES):
            values = both_ref[half, :, start : start + LANES].astype(F32).reshape(rows // 8, 8, LANES)
            values = values - per_part(values)[None]
            spread = per_part(jnp.square(values))
            values = (values * lax.rsqrt(spread + epsilon)[None]).reshape(rows, LANES)
            tnorm = (values * gain + bias).astype(BF16)
            mixing = nn(mixer, tnorm)
            mixed[:, start : start + LANES] = (gating_ref[half, :, start : start + LANES] * mixing).astype(BF16)
        for part in range(2):
            for at in range(deep):
                place = half * 2 * deep + part * deep + at
                update_ref[place] = mixed[part * outs : (part + 1) * outs, at * cols : (at + 1) * cols]
    last = both_ref[0, :, wide - LANES :]
    row = lax.broadcasted_iota(jnp.int32, (rows, outs), 0)
    col = lax.broadcasted_iota(jnp.int32, (rows, outs), 1)
    chosen = jnp.where(row == 2 * (col + half_ref[0] * outs), 1.0, 0.0).astype(BF16)
    sums = lax.dot_general(last, chosen, (((0,), (0,)), ((), ())), preferred_element_type=F32)
    goal = span % LANES
    amax_ref[0:1, :] = sums[goal : goal + 1] + sums[goal + 1 : goal + 2] + sums[goal + 2 : goal + 3]
    amax_ref[1:2, :] = sums[goal + 3 : goal + 4] + sums[goal + 4 : goal + 5] + sums[goal + 5 : goal + 6]


VMEM = pl.BlockSpec(memory_space=pltpu.VMEM)
HBM = pl.BlockSpec(memory_space=pltpu.HBM)
SMEM = pl.BlockSpec(memory_space=pltpu.SMEM)
GRANT = pltpu.CompilerParams(vmem_limit_bytes=24 * 2**20)


def on_device(
    pair_rep,
    pair_mask,
    amax_history,
    in_gain,
    in_bias,
    proj_weight,
    gate_weight,
    out_gain,
    out_bias,
    out_weight,
):
    rows, cols, channels = pair_rep.shape[1:]
    deep = rows // 4
    span = deep * cols
    wide = lane_round(span)
    groups, ranks = lax.axis_size("gy"), lax.axis_size("gx")
    chips = ("gy", "gx")
    assert groups * ranks == channels and lax.axis_size("col") == 2
    half = lax.axis_index("col").reshape(1).astype(jnp.int32)
    rep = pair_rep[0]
    gain, bias = in_gain[None, :], in_bias[None, :]

    packed, near, far, masks = pl.pallas_call(
        prepare_kernel,
        name="prepare",
        out_shape=(
            jax.ShapeDtypeStruct((2 * channels + 16, channels), BF16),
            jax.ShapeDtypeStruct((wide, 2 * channels), BF16),
            jax.ShapeDtypeStruct((wide, 2 * channels), BF16),
            jax.ShapeDtypeStruct((2, 8, wide), F32),
        ),
        in_specs=[SMEM] + [HBM] * 6,
        out_specs=(VMEM,) * 4,
        scratch_shapes=[
            pltpu.VMEM((rows // 2, cols, channels), BF16),
            pltpu.VMEM((rows, cols), jnp.int32),
            pltpu.VMEM((4, channels // 2, channels), BF16),
            pltpu.VMEM((2, channels // 2), F32),
            pltpu.VMEM((1, channels), F32),
            pltpu.VMEM((1, channels), F32),
            pltpu.SemaphoreType.DMA((7,)),
        ],
        compiler_params=GRANT,
    )(half, *map(in_hbm, (rep, pair_mask[0], jnp.transpose(proj_weight, (1, 2, 0)), amax_history, gain, bias)))
    packed = lax.all_gather(packed, "col")
    message = pl.pallas_call(
        functools.partial(project_kernel, span=span),
        name="project",
        out_shape=pltpu.HBM((channels, 2, 2 * wide - LANES), BF16),
        in_specs=[VMEM] * 4,
        out_specs=HBM,
        scratch_shapes=[
            pltpu.VMEM((4, 2 * channels, wide), F32),
            pltpu.VMEM((2 * channels, 2), F32),
            pltpu.VMEM((channels, 2, 2 * wide - LANES), BF16),
            pltpu.SemaphoreType.DMA((channels // 8,)),
        ],
        compiler_params=GRANT,
    )(packed, near, far, masks)
    received = lax.all_to_all(message, chips, split_axis=0, concat_axis=0, tiled=True)
    mine = lax.axis_index(chips).reshape(1).astype(jnp.int32)
    gating, mixer, order, columns, scale = pl.pallas_call(
        gate_kernel,
        name="gate",
        out_shape=(
            jax.ShapeDtypeStruct((2, channels, wide), F32),
            jax.ShapeDtypeStruct((channels, 2 * channels), BF16),
            jax.ShapeDtypeStruct((ranks * rows, groups * LANES), BF16),
            jax.ShapeDtypeStruct((2 * channels, 2), F32),
            jax.ShapeDtypeStruct((8, LANES), F32),
        ),
        in_specs=[SMEM] + [VMEM] * 7,
        out_specs=(VMEM,) * 5,
        scratch_shapes=[pltpu.VMEM((wide, 2 * channels), BF16)],
        compiler_params=GRANT,
        cost_estimate=pl.CostEstimate(flops=20_000_000_000, bytes_accessed=3_000_000, transcendentals=0),
    )(mine, rep, packed, gate_weight.T, out_weight.T, gain, bias, jnp.stack([out_gain, out_bias]))
    count = ranks * rows // 2
    left, right = pl.pallas_call(
        functools.partial(unpack_kernel, groups=groups, deep=deep, cols=cols),
        name="unpack",
        out_shape=(
            jax.ShapeDtypeStruct((count, groups * cols), BF16),
            jax.ShapeDtypeStruct((count + 16, groups * cols), BF16),
        ),
        in_specs=[VMEM],
        out_specs=(VMEM,) * 2,
        scratch_shapes=[pltpu.VMEM((2 * channels, 2 * wide - LANES), BF16)],
        compiler_params=GRANT,
    )(received)
    both = lax.all_gather(right, "col")
    products = pl.pallas_call(
        functools.partial(triangle_kernel, groups=groups, deep=deep, cols=cols),
        name="triangle",
        out_shape=jax.ShapeDtypeStruct((channels, 2, wide), BF16),
        in_specs=[VMEM] * 4,
        out_specs=VMEM,
        scratch_shapes=[pltpu.VMEM((count, groups * LANES), BF16)],
        compiler_params=GRANT,
    )(scale, left, both, order)
    returned = lax.all_to_all(products, chips, split_axis=0, concat_axis=0, tiled=True)
    both = lax.all_gather(returned.reshape(2 * channels, -1), "col")
    update, new_amax = pl.pallas_call(
        functools.partial(finish_kernel, deep=deep, cols=cols),
        name="finish",
        out_shape=(
            jax.ShapeDtypeStruct((rows, channels // 2, cols), BF16),
            jax.ShapeDtypeStruct((2, channels // 2), F32),
        ),
        in_specs=[SMEM] + [VMEM] * 4,
        out_specs=(VMEM,) * 2,
        scratch_shapes=[pltpu.VMEM((channels, wide), BF16)],
        compiler_params=GRANT,
    )(half, both, gating, mixer, columns)
    return (jnp.transpose(update, (0, 2, 1))[None], new_amax)


def solution(mesh):
    placed = (
        P("ga", "gx", "gy", None),
        P("ga", "gx", "gy"),
        P(None, "col"),
        P(),
        P(),
        P(None, None, "col"),
        P(None, "col"),
        P(),
        P(),
        P(None, "col"),
    )
    return jax.shard_map(
        on_device,
        mesh=mesh,
        in_specs=placed,
        out_specs=(P("ga", "gx", "gy", "col"), P("ga", "col")),
        check_vma=False,
    )
```

```python
import functools

import jax
import jax.numpy as jnp
from jax import lax
from jax.experimental import pallas as pl
from jax.experimental.pallas import tpu as pltpu
from jax.sharding import PartitionSpec as P

epsilon = 1e-05
format_limit = 448.0
LANES = 128
F32 = jnp.float32
BF16 = jnp.bfloat16


def lane_round(size):
    return -(-size // LANES) * LANES


def normed_rows(rows, gain, bias):
    average = jnp.mean(rows, axis=-1, keepdims=True)
    spread = jnp.mean(jnp.square(rows - average), axis=-1, keepdims=True)
    return ((rows - average) * lax.rsqrt(spread + epsilon) * gain + bias).astype(BF16)


def one_hot_rows(channels, parity, dtype=BF16):
    row = lax.broadcasted_iota(jnp.int32, (2 * channels, channels), 0)
    col = lax.broadcasted_iota(jnp.int32, (2 * channels, channels), 1)
    return jnp.where(row == 2 * col + parity, 1.0, 0.0).astype(dtype)


def one_hot_cols(channels, parity):
    row = lax.broadcasted_iota(jnp.int32, (channels, 2 * channels), 0)
    col = lax.broadcasted_iota(jnp.int32, (channels, 2 * channels), 1)
    return jnp.where(col == 2 * row + parity, 1.0, 0.0).astype(BF16)


def in_hbm(array):
    return pltpu.with_memory_space_constraint(array, pltpu.HBM)


def nn(left, right):
    return jnp.dot(left, right, preferred_element_type=F32)


def nt(left, right):
    return lax.dot_general(left, right, (((1,), (1,)), ((), ())), preferred_element_type=F32)


def split_parts(values):
    high = values.astype(BF16).astype(F32)
    middle = (values - high).astype(BF16).astype(F32)
    return high, middle, values - high - middle


def columns_of(rows, channels):
    parts = jnp.concatenate([*split_parts(rows), jnp.zeros_like(rows)], axis=0).astype(BF16)
    return columns_of_parts(parts, channels)


def columns_of_parts(parts, channels):
    both = (one_hot_rows(channels, 0, F32) + one_hot_rows(channels, 1, F32)).astype(BF16)
    columns = nt(both, parts)
    return columns[:, 0:2] + columns[:, 2:4] + columns[:, 4:6]


def fetch_kernel(
    half_ref,
    rep_hbm,
    mask_hbm,
    weight_hbm,
    history_hbm,
    gain_hbm,
    bias_hbm,
    packed_ref,
    rep_ref,
    mask_ref,
    affine_ref,
    weight_ref,
    history_ref,
    sems,
):
    which, outs, channels = weight_ref.shape
    held = rep_ref.shape[0]
    copies = [
        pltpu.make_async_copy(source, target, sems.at[at])
        for at, (source, target) in enumerate(
            (
                (weight_hbm, weight_ref),
                (history_hbm, history_ref),
                (rep_hbm.at[pl.ds(half_ref[0] * held, held)], rep_ref),
                (gain_hbm, affine_ref.at[pl.ds(0, 1)]),
                (bias_hbm, affine_ref.at[pl.ds(1, 1)]),
                (mask_hbm, mask_ref),
            )
        )
    ]
    for copy in copies:
        copy.start()
    for copy in copies[:2]:
        copy.wait()
    for at in range(which):
        packed_ref[at * outs : (at + 1) * outs, :] = weight_ref[at]
    history = history_ref[...]
    parts = jnp.concatenate([*split_parts(history), jnp.zeros_like(history)], axis=0)
    parts = jnp.concatenate([parts, jnp.zeros_like(parts)], axis=1)
    parts = jnp.concatenate([parts, jnp.zeros_like(parts)], axis=0)
    packed_ref[which * outs :, :] = parts.astype(BF16)
    for copy in copies[2:]:
        copy.wait()


def norm_kernel(half_ref, rep_ref, mask_ref, affine_ref, near, far, masks_ref):
    held, cols, channels = rep_ref.shape
    deep = held // 2
    span = deep * cols
    wide = near.shape[0]
    shift = span - (wide - LANES)
    near[pl.ds(span, wide - span), :] = jnp.zeros((wide - span, 2 * channels), BF16)
    far[pl.ds(0, shift), :] = jnp.zeros((shift, 2 * channels), BF16)
    far[pl.ds(shift + span, wide - span - shift), :] = jnp.zeros((wide - span - shift, 2 * channels), BF16)
    gain, bias = affine_ref[0:1, :], affine_ref[1:2, :]
    for part in range(2):
        block = rep_ref[part * deep : (part + 1) * deep].reshape(span, channels)
        block = normed_rows(block.astype(F32), gain, bias)
        lanes = slice(part * channels, (part + 1) * channels)
        near[0:span, lanes] = block
        far[shift : shift + span, lanes] = block
    masks = mask_ref[...].astype(F32)
    masks = jnp.where(half_ref[0] == 0, masks[:held], masks[held:])
    pieces = [
        jnp.concatenate([masks[at : at + 1], masks[deep + at : deep + at + 1]], axis=0)
        for at in range(deep)
    ]
    zeros = jnp.zeros((2, wide - span), F32)
    mask_near = jnp.concatenate([jnp.concatenate([*pieces, zeros], axis=1)] * 4, axis=0)
    masks_ref[0] = mask_near
    masks_ref[1] = pltpu.roll(mask_near, shift, 1)


def ordered(half, own_ref, other_ref):
    own, other = own_ref[...].astype(F32), other_ref[...].astype(F32)
    return [jnp.where(half == 0, own, other).astype(BF16), jnp.where(half == 0, other, own).astype(BF16)]


def history_parts(packed, outs):
    start = packed[0].shape[0] - 16
    return jnp.concatenate([held[start:, :outs] for held in packed], axis=1)[:8]


def project_kernel(half_ref, packed_ref, other_ref, near, far, masks_ref, out_hbm, proj, inverse_ref, out_ref, sems, *, span):
    wide, channels = near.shape[0], near.shape[1] // 2
    outs = channels // 2
    shift = span - (wide - LANES)
    packed = ordered(half_ref[0], packed_ref, other_ref)
    inverse_ref[...] = format_limit / columns_of_parts(history_parts(packed, outs), channels)
    even, odd = one_hot_rows(channels, 0), one_hot_rows(channels, 1)
    weight = jnp.concatenate(
        [
            jnp.concatenate([held[at * outs : (at + 1) * outs] for held in packed], axis=0)
            for at in range(4)
        ],
        axis=1,
    )
    evens, odds = nn(even, weight).astype(BF16), nn(odd, weight).astype(BF16)
    for side in range(2):
        both = [
            jnp.concatenate([held[:, at * channels : (at + 1) * channels] for held in (evens, odds)], axis=1)
            for at in (2 * side, 2 * side + 1)
        ]
        values = nt(jnp.concatenate(both, axis=0), (near if side == 0 else far)[...])
        proj[2 * side : 2 * side + 2] = values.reshape(2, 2 * channels, wide)
    mask_near = jnp.concatenate([masks_ref[0]] * 2, axis=0)
    mask_far = jnp.concatenate([masks_ref[1]] * 2, axis=0)
    lane = lax.broadcasted_iota(jnp.int32, (16, LANES), 1)
    first = shift + span - (wide - LANES)

    def step(at, carry):
        rows_at = pl.ds(pl.multiple_of(at * 16, 16), 16)
        left = mask_near * jax.nn.sigmoid(proj[1, rows_at, :]) * proj[0, rows_at, :]
        right = mask_far * jax.nn.sigmoid(proj[3, rows_at, :]) * proj[2, rows_at, :]
        left_max = jnp.max(jnp.abs(left), axis=1, keepdims=True)
        right_max = jnp.max(jnp.abs(right), axis=1, keepdims=True)
        inverse = inverse_ref[rows_at, :]
        left = jnp.clip(left * inverse[:, 0:1], -format_limit, format_limit)
        right = jnp.clip(right * inverse[:, 1:2], -format_limit, format_limit)
        edge = wide - LANES
        peers_at = pl.ds(at * 8, 8)

        def put(start, stop, values):
            out_ref[peers_at, :, start:stop] = values.astype(BF16).reshape(8, 2, stop - start)

        put(0, edge, left[:, :edge])
        put(edge, wide, left[:, edge:] + right[:, :LANES])
        put(wide, wide + edge - LANES, right[:, LANES:edge])
        last = right[:, edge:]
        for place, part in enumerate((*split_parts(left_max), *split_parts(right_max))):
            last = jnp.where(lane == first + place, part, last)
        put(wide + edge - LANES, wide + edge, last)
        sent(at).start()
        return carry

    def sent(at):
        peers_at = pl.ds(at * 8, 8)
        return pltpu.make_async_copy(out_ref.at[peers_at], out_hbm.at[peers_at], sems.at[at])

    def settle(at, carry):
        sent(at).wait()
        return carry

    lax.fori_loop(0, channels // 8, step, 0, unroll=8)
    lax.fori_loop(0, channels // 8, settle, 0)


def gate_kernel(
    half_ref,
    mine_ref,
    rep_ref,
    packed_ref,
    other_ref,
    gate_ref,
    weight_ref,
    gain_ref,
    bias_ref,
    affine_ref,
    gating_ref,
    mixer_ref,
    order_ref,
    columns_ref,
    scale_ref,
    near,
):
    rows, cols, channels = rep_ref.shape
    deep = rows // 4
    span = deep * cols
    outs = gate_ref.shape[0]
    gain, bias = gain_ref[...], bias_ref[...]
    blank = jnp.zeros((outs, channels), BF16)
    gate = gate_ref[...]
    wide_gate = jnp.concatenate(
        [jnp.concatenate([gate, blank], axis=1), jnp.concatenate([blank, gate], axis=1)], axis=0
    )
    near[span:, :] = jnp.zeros((near.shape[0] - span, 2 * channels), BF16)
    for half in range(2):
        for part in range(2):
            start = half * (2 * deep) + part * deep
            block = rep_ref[start : start + deep].reshape(span, channels).astype(F32)
            near[0:span, part * channels : (part + 1) * channels] = normed_rows(block, gain, bias)
        gating_ref[half] = jax.nn.sigmoid(nt(wide_gate, near[...]))
    columns_ref[...] = columns_of(affine_ref[...], channels)
    parts = history_parts(ordered(half_ref[0], packed_ref, other_ref), outs).astype(F32)
    lane = lax.broadcasted_iota(jnp.int32, parts.shape, 1)
    parts = jnp.sum(jnp.where(lane == mine_ref[0], parts, 0.0), axis=1, keepdims=True)
    scales = (parts[0:2] + parts[2:4] + parts[4:6]) / format_limit
    scale_ref[...] = jnp.broadcast_to(scales[0:1] * scales[1:2], scale_ref.shape)
    weight = weight_ref[...]
    mixer_ref[0:outs, :] = nn(weight, one_hot_cols(channels, 0)).astype(BF16)
    mixer_ref[outs:, :] = nn(weight, one_hot_cols(channels, 1)).astype(BF16)
    count, lanes = order_ref.shape
    per_half = count // 2
    per_at = per_half // deep
    pairs = cols // rows
    step = 32
    for start in range(0, count, step):
        row = start + lax.broadcasted_iota(jnp.int32, (step, 1), 0)
        half_at = start // per_half
        deep_at = (start % per_half) // per_at
        block = (row - half_at * per_half - deep_at * per_at) >> 1
        part = row & 1
        target = (block // pairs) * LANES + (block % pairs) * rows + half_at * 2 * deep + part * deep + deep_at
        lane = lax.broadcasted_iota(jnp.int32, (step, lanes), 1)
        order_ref[start : start + step, :] = jnp.where(lane == target, 1.0, 0.0).astype(BF16)


def unpack_kernel(received_ref, left_ref, right_ref, flat, *, groups, deep, cols):
    rows, lanes = flat.shape
    block = rows // groups
    span = deep * cols
    for group in range(groups):
        piece = received_ref[group * block // 2 : (group + 1) * block // 2]
        flat[group * block : (group + 1) * block, :] = piece.reshape(block, lanes)

    def window(group, start):
        base = start // LANES * LANES
        stop = -(-(start + cols) // LANES) * LANES
        return flat[group * block : (group + 1) * block, base:stop][:, start - base : start - base + cols]

    for at in range(deep):
        place = pl.ds(at * block, block)
        left_ref[place, :] = jnp.concatenate([window(g, at * cols) for g in range(groups)], axis=1)
        right_ref[place, :] = jnp.concatenate([window(g, span + at * cols) for g in range(groups)], axis=1)
    parts = flat[:, lanes - LANES :].astype(F32)
    total = parts + pltpu.roll(parts, LANES - 1, 1) + pltpu.roll(parts, LANES - 2, 1)
    best = jnp.max(jnp.max(total.reshape(rows // 8, 8, LANES), axis=0), axis=0, keepdims=True)
    best = jnp.concatenate([*split_parts(best), jnp.zeros((13, LANES), F32)], axis=0).astype(BF16)
    right_ref[deep * block :, :] = jnp.concatenate(
        [best, jnp.zeros((16, groups * cols - LANES), BF16)], axis=1
    )


def triangle_kernel(scale_ref, left_ref, both_ref, order_ref, out_ref, moved, *, groups, deep, cols):
    count = left_ref.shape[0]
    block = count // deep
    span = deep * cols
    scale = scale_ref[0:1, 0:1]
    best = None
    for other in range(2):
        parts = both_ref[other, count:, :LANES].astype(F32)
        parts = parts[0:1] + parts[1:2] + parts[2:3]
        best = parts if best is None else jnp.maximum(best, parts)
    right = jnp.concatenate([both_ref[other, :count, :] for other in range(2)], axis=0)
    products = nt(left_ref[...], right) * scale
    moved[...] = nn(products.astype(BF16), order_ref[...]).astype(BF16)
    lane = lax.broadcasted_iota(jnp.int32, (8, LANES), 1)
    first = 2 * span % LANES
    goal = span % LANES
    best = jnp.broadcast_to(best, (8, LANES))
    tail = jnp.zeros((8, LANES), F32)
    for place, part in enumerate(split_parts(best)):
        turned = pltpu.roll(part, (goal + place - first) % LANES, 1)
        tail = jnp.where((lane == goal + place) | (lane == goal + place + 3), turned, tail)
    tail = jnp.broadcast_to(tail[0:1, goal:], (block, LANES - goal)).astype(BF16)
    for group in range(groups):
        pieces = [
            moved[at * block : (at + 1) * block, group * LANES : group * LANES + cols] for at in range(deep)
        ]
        pieces = jnp.concatenate([*pieces, tail], axis=1)
        out_ref[group * block // 2 : (group + 1) * block // 2] = pieces.reshape(block // 2, 2, -1)


def finish_kernel(
    half_ref, both_ref, gating_ref, mixer_ref, columns_ref, update_ref, amax_ref, mixed, *, deep, cols
):
    rows, wide = both_ref.shape[1:]
    channels = rows // 2
    outs = update_ref.shape[1]
    span = deep * cols
    gain, bias = columns_ref[:, 0:1], columns_ref[:, 1:2]
    mixer = mixer_ref[...]

    def per_part(values):
        total = jnp.sum(values, axis=0)
        total = total + pltpu.roll(total, 4, 0)
        total = total + pltpu.roll(total, 2, 0)
        return total * (1.0 / channels)

    for half in range(2):
        for start in range(0, wide, LANES):
            values = both_ref[half, :, start : start + LANES].astype(F32).reshape(rows // 8, 8, LANES)
            values = values - per_part(values)[None]
            spread = per_part(jnp.square(values))
            values = (values * lax.rsqrt(spread + epsilon)[None]).reshape(rows, LANES)
            tnorm = (values * gain + bias).astype(BF16)
            mixing = nn(mixer, tnorm)
            mixed[:, start : start + LANES] = (gating_ref[half, :, start : start + LANES] * mixing).astype(BF16)
        for part in range(2):
            for at in range(deep):
                place = half * 2 * deep + part * deep + at
                update_ref[place] = mixed[part * outs : (part + 1) * outs, at * cols : (at + 1) * cols]
    last = both_ref[0, :, wide - LANES :]
    row = lax.broadcasted_iota(jnp.int32, (rows, outs), 0)
    col = lax.broadcasted_iota(jnp.int32, (rows, outs), 1)
    chosen = jnp.where(row == 2 * (col + half_ref[0] * outs), 1.0, 0.0).astype(BF16)
    sums = lax.dot_general(last, chosen, (((0,), (0,)), ((), ())), preferred_element_type=F32)
    goal = span % LANES
    amax_ref[0:1, :] = sums[goal : goal + 1] + sums[goal + 1 : goal + 2] + sums[goal + 2 : goal + 3]
    amax_ref[1:2, :] = sums[goal + 3 : goal + 4] + sums[goal + 4 : goal + 5] + sums[goal + 5 : goal + 6]


VMEM = pl.BlockSpec(memory_space=pltpu.VMEM)
HBM = pl.BlockSpec(memory_space=pltpu.HBM)
SMEM = pl.BlockSpec(memory_space=pltpu.SMEM)
GRANT = pltpu.CompilerParams(vmem_limit_bytes=24 * 2**20)


def on_device(
    pair_rep,
    pair_mask,
    amax_history,
    in_gain,
    in_bias,
    proj_weight,
    gate_weight,
    out_gain,
    out_bias,
    out_weight,
):
    rows, cols, channels = pair_rep.shape[1:]
    deep = rows // 4
    span = deep * cols
    wide = lane_round(span)
    groups, ranks = lax.axis_size("gy"), lax.axis_size("gx")
    chips = ("gy", "gx")
    assert groups * ranks == channels and lax.axis_size("col") == 2
    half = lax.axis_index("col").reshape(1).astype(jnp.int32)
    rep = pair_rep[0]
    gain, bias = in_gain[None, :], in_bias[None, :]

    packed, held, mask, affine = pl.pallas_call(
        fetch_kernel,
        name="fetch",
        out_shape=(
            jax.ShapeDtypeStruct((2 * channels + 16, channels), BF16),
            jax.ShapeDtypeStruct((rows // 2, cols, channels), BF16),
            jax.ShapeDtypeStruct((rows, cols), jnp.int32),
            jax.ShapeDtypeStruct((2, channels), F32),
        ),
        in_specs=[SMEM] + [HBM] * 6,
        out_specs=(VMEM,) * 4,
        scratch_shapes=[
            pltpu.VMEM((4, channels // 2, channels), BF16),
            pltpu.VMEM((2, channels // 2), F32),
            pltpu.SemaphoreType.DMA((6,)),
        ],
        compiler_params=GRANT,
    )(half, *map(in_hbm, (rep, pair_mask[0], jnp.transpose(proj_weight, (1, 2, 0)), amax_history, gain, bias)))
    other = lax.ppermute(packed, "col", [(0, 1), (1, 0)])
    near, far, masks = pl.pallas_call(
        norm_kernel,
        name="norm",
        out_shape=(
            jax.ShapeDtypeStruct((wide, 2 * channels), BF16),
            jax.ShapeDtypeStruct((wide, 2 * channels), BF16),
            jax.ShapeDtypeStruct((2, 8, wide), F32),
        ),
        in_specs=[SMEM] + [VMEM] * 3,
        out_specs=(VMEM,) * 3,
        compiler_params=GRANT,
        cost_estimate=pl.CostEstimate(flops=20_000_000_000, bytes_accessed=3_000_000, transcendentals=0),
    )(half, held, mask, affine)
    message = pl.pallas_call(
        functools.partial(project_kernel, span=span),
        name="project",
        out_shape=pltpu.HBM((channels, 2, 2 * wide - LANES), BF16),
        in_specs=[SMEM] + [VMEM] * 5,
        out_specs=HBM,
        scratch_shapes=[
            pltpu.VMEM((4, 2 * channels, wide), F32),
            pltpu.VMEM((2 * channels, 2), F32),
            pltpu.VMEM((channels, 2, 2 * wide - LANES), BF16),
            pltpu.SemaphoreType.DMA((channels // 8,)),
        ],
        compiler_params=GRANT,
    )(half, packed, other, near, far, masks)
    received = lax.all_to_all(message, chips, split_axis=0, concat_axis=0, tiled=True)
    mine = lax.axis_index(chips).reshape(1).astype(jnp.int32)
    gating, mixer, order, columns, scale = pl.pallas_call(
        gate_kernel,
        name="gate",
        out_shape=(
            jax.ShapeDtypeStruct((2, channels, wide), F32),
            jax.ShapeDtypeStruct((channels, 2 * channels), BF16),
            jax.ShapeDtypeStruct((ranks * rows, groups * LANES), BF16),
            jax.ShapeDtypeStruct((2 * channels, 2), F32),
            jax.ShapeDtypeStruct((8, LANES), F32),
        ),
        in_specs=[SMEM] * 2 + [VMEM] * 8,
        out_specs=(VMEM,) * 5,
        scratch_shapes=[pltpu.VMEM((wide, 2 * channels), BF16)],
        compiler_params=GRANT,
        cost_estimate=pl.CostEstimate(flops=20_000_000_000, bytes_accessed=3_000_000, transcendentals=0),
    )(half, mine, rep, packed, other, gate_weight.T, out_weight.T, gain, bias, jnp.stack([out_gain, out_bias]))
    count = ranks * rows // 2
    left, right = pl.pallas_call(
        functools.partial(unpack_kernel, groups=groups, deep=deep, cols=cols),
        name="unpack",
        out_shape=(
            jax.ShapeDtypeStruct((count, groups * cols), BF16),
            jax.ShapeDtypeStruct((count + 16, groups * cols), BF16),
        ),
        in_specs=[VMEM],
        out_specs=(VMEM,) * 2,
        scratch_shapes=[pltpu.VMEM((2 * channels, 2 * wide - LANES), BF16)],
        compiler_params=GRANT,
    )(received)
    both = lax.all_gather(right, "col")
    products = pl.pallas_call(
        functools.partial(triangle_kernel, groups=groups, deep=deep, cols=cols),
        name="triangle",
        out_shape=jax.ShapeDtypeStruct((channels, 2, wide), BF16),
        in_specs=[VMEM] * 4,
        out_specs=VMEM,
        scratch_shapes=[pltpu.VMEM((count, groups * LANES), BF16)],
        compiler_params=GRANT,
    )(scale, left, both, order)
    returned = lax.all_to_all(products, chips, split_axis=0, concat_axis=0, tiled=True)
    both = lax.all_gather(returned.reshape(2 * channels, -1), "col")
    update, new_amax = pl.pallas_call(
        functools.partial(finish_kernel, deep=deep, cols=cols),
        name="finish",
        out_shape=(
            jax.ShapeDtypeStruct((rows, channels // 2, cols), BF16),
            jax.ShapeDtypeStruct((2, channels // 2), F32),
        ),
        in_specs=[SMEM] + [VMEM] * 4,
        out_specs=(VMEM,) * 2,
        scratch_shapes=[pltpu.VMEM((channels, wide), BF16)],
        compiler_params=GRANT,
    )(half, both, gating, mixer, columns)
    return (jnp.transpose(update, (0, 2, 1))[None], new_amax)


def solution(mesh):
    placed = (
        P("ga", "gx", "gy", None),
        P("ga", "gx", "gy"),
        P(None, "col"),
        P(),
        P(),
        P(None, None, "col"),
        P(None, "col"),
        P(),
        P(),
        P(None, "col"),
    )
    return jax.shard_map(
        on_device,
        mesh=mesh,
        in_specs=placed,
        out_specs=(P("ga", "gx", "gy", "col"), P("ga", "col")),
        check_vma=False,
    )
```

```python
import functools

import jax
import jax.numpy as jnp
from jax import lax
from jax.experimental import pallas as pl
from jax.experimental.pallas import tpu as pltpu
from jax.sharding import PartitionSpec as P

epsilon = 1e-05
format_limit = 448.0
LANES = 128
F32 = jnp.float32
BF16 = jnp.bfloat16


def lane_round(size):
    return -(-size // LANES) * LANES


def normed_rows(rows, gain, bias):
    average = jnp.mean(rows, axis=-1, keepdims=True)
    spread = jnp.mean(jnp.square(rows - average), axis=-1, keepdims=True)
    return ((rows - average) * lax.rsqrt(spread + epsilon) * gain + bias).astype(BF16)


def one_hot_rows(channels, parity, dtype=BF16):
    row = lax.broadcasted_iota(jnp.int32, (2 * channels, channels), 0)
    col = lax.broadcasted_iota(jnp.int32, (2 * channels, channels), 1)
    return jnp.where(row == 2 * col + parity, 1.0, 0.0).astype(dtype)


def one_hot_cols(channels, parity):
    row = lax.broadcasted_iota(jnp.int32, (channels, 2 * channels), 0)
    col = lax.broadcasted_iota(jnp.int32, (channels, 2 * channels), 1)
    return jnp.where(col == 2 * row + parity, 1.0, 0.0).astype(BF16)


def in_hbm(array):
    return pltpu.with_memory_space_constraint(array, pltpu.HBM)


def nn(left, right):
    return jnp.dot(left, right, preferred_element_type=F32)


def nt(left, right):
    return lax.dot_general(left, right, (((1,), (1,)), ((), ())), preferred_element_type=F32)


def split_parts(values):
    high = values.astype(BF16).astype(F32)
    middle = (values - high).astype(BF16).astype(F32)
    return high, middle, values - high - middle


def columns_of(rows, channels):
    parts = jnp.concatenate([*split_parts(rows), jnp.zeros_like(rows)], axis=0).astype(BF16)
    return columns_of_parts(parts, channels)


def columns_of_parts(parts, channels):
    both = (one_hot_rows(channels, 0, F32) + one_hot_rows(channels, 1, F32)).astype(BF16)
    columns = nt(both, parts)
    return columns[:, 0:2] + columns[:, 2:4] + columns[:, 4:6]


def fetch_kernel(
    half_ref,
    rep_hbm,
    mask_hbm,
    weight_hbm,
    history_hbm,
    gain_hbm,
    bias_hbm,
    packed_ref,
    rep_ref,
    mask_ref,
    affine_ref,
    weight_ref,
    history_ref,
    sems,
):
    which, outs, channels = weight_ref.shape
    held = rep_ref.shape[0]
    copies = [
        pltpu.make_async_copy(source, target, sems.at[at])
        for at, (source, target) in enumerate(
            (
                (weight_hbm, weight_ref),
                (history_hbm, history_ref),
                (rep_hbm.at[pl.ds(half_ref[0] * held, held)], rep_ref),
                (gain_hbm, affine_ref.at[pl.ds(0, 1)]),
                (bias_hbm, affine_ref.at[pl.ds(1, 1)]),
                (mask_hbm, mask_ref),
            )
        )
    ]
    for copy in copies:
        copy.start()
    for copy in copies[:2]:
        copy.wait()
    for at in range(which):
        packed_ref[at * outs : (at + 1) * outs, :] = weight_ref[at]
    history = history_ref[...]
    parts = jnp.concatenate([*split_parts(history), jnp.zeros_like(history)], axis=0)
    parts = jnp.concatenate([parts, jnp.zeros_like(parts)], axis=1)
    parts = jnp.concatenate([parts, jnp.zeros_like(parts)], axis=0)
    packed_ref[which * outs :, :] = parts.astype(BF16)
    for copy in copies[2:]:
        copy.wait()


def history_parts(packed_ref, outs):
    start = packed_ref.shape[1] - 16
    pieces = [packed_ref[col, start:, :][:, :outs] for col in range(2)]
    return jnp.concatenate(pieces, axis=1)[:8]


def project_kernel(
    half_ref, packed_ref, rep_ref, mask_ref, affine_ref, out_hbm, near, far, proj, inverse_ref, out_ref, sems
):
    held, cols, channels = rep_ref.shape
    deep = held // 2
    span = deep * cols
    wide = near.shape[0]
    shift = span - (wide - LANES)
    near[pl.ds(span, wide - span), :] = jnp.zeros((wide - span, 2 * channels), BF16)
    far[pl.ds(0, shift), :] = jnp.zeros((shift, 2 * channels), BF16)
    far[pl.ds(shift + span, wide - span - shift), :] = jnp.zeros((wide - span - shift, 2 * channels), BF16)
    gain, bias = affine_ref[0:1, :], affine_ref[1:2, :]
    for part in range(2):
        block = rep_ref[part * deep : (part + 1) * deep].reshape(span, channels)
        block = normed_rows(block.astype(F32), gain, bias)
        lanes = slice(part * channels, (part + 1) * channels)
        near[0:span, lanes] = block
        far[shift : shift + span, lanes] = block
    masks = mask_ref[...].astype(F32)
    masks = jnp.where(half_ref[0] == 0, masks[:held], masks[held:])
    pieces = [
        jnp.concatenate([masks[at : at + 1], masks[deep + at : deep + at + 1]], axis=0)
        for at in range(deep)
    ]
    zeros = jnp.zeros((2, wide - span), F32)
    mask_near = jnp.concatenate([jnp.concatenate([*pieces, zeros], axis=1)] * 4, axis=0)
    mask_far = jnp.concatenate([pltpu.roll(mask_near, shift, 1)] * 2, axis=0)
    mask_near = jnp.concatenate([mask_near] * 2, axis=0)
    outs = channels // 2
    inverse_ref[...] = format_limit / columns_of_parts(history_parts(packed_ref, outs), channels)
    even, odd = one_hot_rows(channels, 0), one_hot_rows(channels, 1)
    weight = jnp.concatenate(
        [
            jnp.concatenate([packed_ref[0, at * outs : (at + 1) * outs], packed_ref[1, at * outs : (at + 1) * outs]], axis=0)
            for at in range(4)
        ],
        axis=1,
    )
    evens, odds = nn(even, weight).astype(BF16), nn(odd, weight).astype(BF16)
    for side in range(2):
        both = [
            jnp.concatenate([held[:, at * channels : (at + 1) * channels] for held in (evens, odds)], axis=1)
            for at in (2 * side, 2 * side + 1)
        ]
        values = nt(jnp.concatenate(both, axis=0), (near if side == 0 else far)[...])
        proj[2 * side : 2 * side + 2] = values.reshape(2, 2 * channels, wide)
    lane = lax.broadcasted_iota(jnp.int32, (16, LANES), 1)
    first = shift + span - (wide - LANES)

    def step(at, carry):
        rows_at = pl.ds(pl.multiple_of(at * 16, 16), 16)
        left = mask_near * jax.nn.sigmoid(proj[1, rows_at, :]) * proj[0, rows_at, :]
        right = mask_far * jax.nn.sigmoid(proj[3, rows_at, :]) * proj[2, rows_at, :]
        left_max = jnp.max(jnp.abs(left), axis=1, keepdims=True)
        right_max = jnp.max(jnp.abs(right), axis=1, keepdims=True)
        inverse = inverse_ref[rows_at, :]
        left = jnp.clip(left * inverse[:, 0:1], -format_limit, format_limit)
        right = jnp.clip(right * inverse[:, 1:2], -format_limit, format_limit)
        edge = wide - LANES
        peers_at = pl.ds(at * 8, 8)

        def put(start, stop, values):
            out_ref[peers_at, :, start:stop] = values.astype(BF16).reshape(8, 2, stop - start)

        put(0, edge, left[:, :edge])
        put(edge, wide, left[:, edge:] + right[:, :LANES])
        put(wide, wide + edge - LANES, right[:, LANES:edge])
        last = right[:, edge:]
        for place, part in enumerate((*split_parts(left_max), *split_parts(right_max))):
            last = jnp.where(lane == first + place, part, last)
        put(wide + edge - LANES, wide + edge, last)
        sent(at).start()
        return carry

    def sent(at):
        peers_at = pl.ds(at * 8, 8)
        return pltpu.make_async_copy(out_ref.at[peers_at], out_hbm.at[peers_at], sems.at[at])

    def settle(at, carry):
        sent(at).wait()
        return carry

    lax.fori_loop(0, channels // 8, step, 0, unroll=8)
    lax.fori_loop(0, channels // 8, settle, 0)


def gate_kernel(
    mine_ref,
    rep_ref,
    packed_ref,
    gate_ref,
    weight_ref,
    gain_ref,
    bias_ref,
    affine_ref,
    gating_ref,
    mixer_ref,
    order_ref,
    columns_ref,
    scale_ref,
    near,
):
    rows, cols, channels = rep_ref.shape
    deep = rows // 4
    span = deep * cols
    outs = gate_ref.shape[0]
    gain, bias = gain_ref[...], bias_ref[...]
    blank = jnp.zeros((outs, channels), BF16)
    gate = gate_ref[...]
    wide_gate = jnp.concatenate(
        [jnp.concatenate([gate, blank], axis=1), jnp.concatenate([blank, gate], axis=1)], axis=0
    )
    near[span:, :] = jnp.zeros((near.shape[0] - span, 2 * channels), BF16)
    for half in range(2):
        for part in range(2):
            start = half * (2 * deep) + part * deep
            block = rep_ref[start : start + deep].reshape(span, channels).astype(F32)
            near[0:span, part * channels : (part + 1) * channels] = normed_rows(block, gain, bias)
        gating_ref[half] = jax.nn.sigmoid(nt(wide_gate, near[...]))
    columns_ref[...] = columns_of(affine_ref[...], channels)
    parts = history_parts(packed_ref, outs).astype(F32)
    lane = lax.broadcasted_iota(jnp.int32, parts.shape, 1)
    parts = jnp.sum(jnp.where(lane == mine_ref[0], parts, 0.0), axis=1, keepdims=True)
    scales = (parts[0:2] + parts[2:4] + parts[4:6]) / format_limit
    scale_ref[...] = jnp.broadcast_to(scales[0:1] * scales[1:2], scale_ref.shape)
    weight = weight_ref[...]
    mixer_ref[0:outs, :] = nn(weight, one_hot_cols(channels, 0)).astype(BF16)
    mixer_ref[outs:, :] = nn(weight, one_hot_cols(channels, 1)).astype(BF16)
    count, lanes = order_ref.shape
    per_half = count // 2
    per_at = per_half // deep
    pairs = cols // rows
    step = 32
    for start in range(0, count, step):
        row = start + lax.broadcasted_iota(jnp.int32, (step, 1), 0)
        half_at = start // per_half
        deep_at = (start % per_half) // per_at
        block = (row - half_at * per_half - deep_at * per_at) >> 1
        part = row & 1
        target = (block // pairs) * LANES + (block % pairs) * rows + half_at * 2 * deep + part * deep + deep_at
        lane = lax.broadcasted_iota(jnp.int32, (step, lanes), 1)
        order_ref[start : start + step, :] = jnp.where(lane == target, 1.0, 0.0).astype(BF16)


def unpack_kernel(received_ref, left_ref, right_ref, flat, *, groups, deep, cols):
    rows, lanes = flat.shape
    block = rows // groups
    span = deep * cols
    for group in range(groups):
        piece = received_ref[group * block // 2 : (group + 1) * block // 2]
        flat[group * block : (group + 1) * block, :] = piece.reshape(block, lanes)

    def window(group, start):
        base = start // LANES * LANES
        stop = -(-(start + cols) // LANES) * LANES
        return flat[group * block : (group + 1) * block, base:stop][:, start - base : start - base + cols]

    for at in range(deep):
        place = pl.ds(at * block, block)
        left_ref[place, :] = jnp.concatenate([window(g, at * cols) for g in range(groups)], axis=1)
        right_ref[place, :] = jnp.concatenate([window(g, span + at * cols) for g in range(groups)], axis=1)
    parts = flat[:, lanes - LANES :].astype(F32)
    total = parts + pltpu.roll(parts, LANES - 1, 1) + pltpu.roll(parts, LANES - 2, 1)
    best = jnp.max(jnp.max(total.reshape(rows // 8, 8, LANES), axis=0), axis=0, keepdims=True)
    best = jnp.concatenate([*split_parts(best), jnp.zeros((13, LANES), F32)], axis=0).astype(BF16)
    right_ref[deep * block :, :] = jnp.concatenate(
        [best, jnp.zeros((16, groups * cols - LANES), BF16)], axis=1
    )


def triangle_kernel(scale_ref, left_ref, both_ref, order_ref, out_ref, moved, *, groups, deep, cols):
    count = left_ref.shape[0]
    block = count // deep
    span = deep * cols
    scale = scale_ref[0:1, 0:1]
    best = None
    for other in range(2):
        parts = both_ref[other, count:, :LANES].astype(F32)
        parts = parts[0:1] + parts[1:2] + parts[2:3]
        best = parts if best is None else jnp.maximum(best, parts)
    right = jnp.concatenate([both_ref[other, :count, :] for other in range(2)], axis=0)
    products = nt(left_ref[...], right) * scale
    moved[...] = nn(products.astype(BF16), order_ref[...]).astype(BF16)
    lane = lax.broadcasted_iota(jnp.int32, (8, LANES), 1)
    first = 2 * span % LANES
    goal = span % LANES
    best = jnp.broadcast_to(best, (8, LANES))
    tail = jnp.zeros((8, LANES), F32)
    for place, part in enumerate(split_parts(best)):
        turned = pltpu.roll(part, (goal + place - first) % LANES, 1)
        tail = jnp.where((lane == goal + place) | (lane == goal + place + 3), turned, tail)
    tail = jnp.broadcast_to(tail[0:1, goal:], (block, LANES - goal)).astype(BF16)
    for group in range(groups):
        pieces = [
            moved[at * block : (at + 1) * block, group * LANES : group * LANES + cols] for at in range(deep)
        ]
        pieces = jnp.concatenate([*pieces, tail], axis=1)
        out_ref[group * block // 2 : (group + 1) * block // 2] = pieces.reshape(block // 2, 2, -1)


def finish_kernel(
    half_ref, both_ref, gating_ref, mixer_ref, columns_ref, update_ref, amax_ref, mixed, *, deep, cols
):
    rows, wide = both_ref.shape[1:]
    channels = rows // 2
    outs = update_ref.shape[1]
    span = deep * cols
    gain, bias = columns_ref[:, 0:1], columns_ref[:, 1:2]
    mixer = mixer_ref[...]

    def per_part(values):
        total = jnp.sum(values, axis=0)
        total = total + pltpu.roll(total, 4, 0)
        total = total + pltpu.roll(total, 2, 0)
        return total * (1.0 / channels)

    for half in range(2):
        for start in range(0, wide, LANES):
            values = both_ref[half, :, start : start + LANES].astype(F32).reshape(rows // 8, 8, LANES)
            values = values - per_part(values)[None]
            spread = per_part(jnp.square(values))
            values = (values * lax.rsqrt(spread + epsilon)[None]).reshape(rows, LANES)
            tnorm = (values * gain + bias).astype(BF16)
            mixing = nn(mixer, tnorm)
            mixed[:, start : start + LANES] = (gating_ref[half, :, start : start + LANES] * mixing).astype(BF16)
        for part in range(2):
            for at in range(deep):
                place = half * 2 * deep + part * deep + at
                update_ref[place] = mixed[part * outs : (part + 1) * outs, at * cols : (at + 1) * cols]
    last = both_ref[0, :, wide - LANES :]
    row = lax.broadcasted_iota(jnp.int32, (rows, outs), 0)
    col = lax.broadcasted_iota(jnp.int32, (rows, outs), 1)
    chosen = jnp.where(row == 2 * (col + half_ref[0] * outs), 1.0, 0.0).astype(BF16)
    sums = lax.dot_general(last, chosen, (((0,), (0,)), ((), ())), preferred_element_type=F32)
    goal = span % LANES
    amax_ref[0:1, :] = sums[goal : goal + 1] + sums[goal + 1 : goal + 2] + sums[goal + 2 : goal + 3]
    amax_ref[1:2, :] = sums[goal + 3 : goal + 4] + sums[goal + 4 : goal + 5] + sums[goal + 5 : goal + 6]


VMEM = pl.BlockSpec(memory_space=pltpu.VMEM)
HBM = pl.BlockSpec(memory_space=pltpu.HBM)
SMEM = pl.BlockSpec(memory_space=pltpu.SMEM)
GRANT = pltpu.CompilerParams(vmem_limit_bytes=24 * 2**20)


def on_device(
    pair_rep,
    pair_mask,
    amax_history,
    in_gain,
    in_bias,
    proj_weight,
    gate_weight,
    out_gain,
    out_bias,
    out_weight,
):
    rows, cols, channels = pair_rep.shape[1:]
    deep = rows // 4
    span = deep * cols
    wide = lane_round(span)
    groups, ranks = lax.axis_size("gy"), lax.axis_size("gx")
    chips = ("gy", "gx")
    assert groups * ranks == channels and lax.axis_size("col") == 2
    half = lax.axis_index("col").reshape(1).astype(jnp.int32)
    rep = pair_rep[0]
    gain, bias = in_gain[None, :], in_bias[None, :]

    packed, held, mask, affine = pl.pallas_call(
        fetch_kernel,
        name="fetch",
        out_shape=(
            jax.ShapeDtypeStruct((2 * channels + 16, channels), BF16),
            jax.ShapeDtypeStruct((rows // 2, cols, channels), BF16),
            jax.ShapeDtypeStruct((rows, cols), jnp.int32),
            jax.ShapeDtypeStruct((2, channels), F32),
        ),
        in_specs=[SMEM] + [HBM] * 6,
        out_specs=(VMEM,) * 4,
        scratch_shapes=[
            pltpu.VMEM((4, channels // 2, channels), BF16),
            pltpu.VMEM((2, channels // 2), F32),
            pltpu.SemaphoreType.DMA((6,)),
        ],
        compiler_params=GRANT,
    )(half, *map(in_hbm, (rep, pair_mask[0], jnp.transpose(proj_weight, (1, 2, 0)), amax_history, gain, bias)))
    packed = lax.all_gather(packed, "col")
    message = pl.pallas_call(
        project_kernel,
        name="project",
        out_shape=pltpu.HBM((channels, 2, 2 * wide - LANES), BF16),
        in_specs=[SMEM] + [VMEM] * 4,
        out_specs=HBM,
        scratch_shapes=[
            pltpu.VMEM((wide, 2 * channels), BF16),
            pltpu.VMEM((wide, 2 * channels), BF16),
            pltpu.VMEM((4, 2 * channels, wide), F32),
            pltpu.VMEM((2 * channels, 2), F32),
            pltpu.VMEM((channels, 2, 2 * wide - LANES), BF16),
            pltpu.SemaphoreType.DMA((channels // 8,)),
        ],
        compiler_params=GRANT,
    )(half, packed, held, mask, affine)
    received = lax.all_to_all(message, chips, split_axis=0, concat_axis=0, tiled=True)
    mine = lax.axis_index(chips).reshape(1).astype(jnp.int32)
    gating, mixer, order, columns, scale = pl.pallas_call(
        gate_kernel,
        name="gate",
        out_shape=(
            jax.ShapeDtypeStruct((2, channels, wide), F32),
            jax.ShapeDtypeStruct((channels, 2 * channels), BF16),
            jax.ShapeDtypeStruct((ranks * rows, groups * LANES), BF16),
            jax.ShapeDtypeStruct((2 * channels, 2), F32),
            jax.ShapeDtypeStruct((8, LANES), F32),
        ),
        in_specs=[SMEM] + [VMEM] * 7,
        out_specs=(VMEM,) * 5,
        scratch_shapes=[pltpu.VMEM((wide, 2 * channels), BF16)],
        compiler_params=GRANT,
        cost_estimate=pl.CostEstimate(flops=20_000_000_000, bytes_accessed=3_000_000, transcendentals=0),
    )(mine, rep, packed, gate_weight.T, out_weight.T, gain, bias, jnp.stack([out_gain, out_bias]))
    count = ranks * rows // 2
    left, right = pl.pallas_call(
        functools.partial(unpack_kernel, groups=groups, deep=deep, cols=cols),
        name="unpack",
        out_shape=(
            jax.ShapeDtypeStruct((count, groups * cols), BF16),
            jax.ShapeDtypeStruct((count + 16, groups * cols), BF16),
        ),
        in_specs=[VMEM],
        out_specs=(VMEM,) * 2,
        scratch_shapes=[pltpu.VMEM((2 * channels, 2 * wide - LANES), BF16)],
        compiler_params=GRANT,
    )(received)
    both = lax.all_gather(right, "col")
    products = pl.pallas_call(
        functools.partial(triangle_kernel, groups=groups, deep=deep, cols=cols),
        name="triangle",
        out_shape=jax.ShapeDtypeStruct((channels, 2, wide), BF16),
        in_specs=[VMEM] * 4,
        out_specs=VMEM,
        scratch_shapes=[pltpu.VMEM((count, groups * LANES), BF16)],
        compiler_params=GRANT,
    )(scale, left, both, order)
    returned = lax.all_to_all(products, chips, split_axis=0, concat_axis=0, tiled=True)
    both = lax.all_gather(returned.reshape(2 * channels, -1), "col")
    update, new_amax = pl.pallas_call(
        functools.partial(finish_kernel, deep=deep, cols=cols),
        name="finish",
        out_shape=(
            jax.ShapeDtypeStruct((rows, channels // 2, cols), BF16),
            jax.ShapeDtypeStruct((2, channels // 2), F32),
        ),
        in_specs=[SMEM] + [VMEM] * 4,
        out_specs=(VMEM,) * 2,
        scratch_shapes=[pltpu.VMEM((channels, wide), BF16)],
        compiler_params=GRANT,
    )(half, both, gating, mixer, columns)
    return (jnp.transpose(update, (0, 2, 1))[None], new_amax)


def solution(mesh):
    placed = (
        P("ga", "gx", "gy", None),
        P("ga", "gx", "gy"),
        P(None, "col"),
        P(),
        P(),
        P(None, None, "col"),
        P(None, "col"),
        P(),
        P(),
        P(None, "col"),
    )
    return jax.shard_map(
        on_device,
        mesh=mesh,
        in_specs=placed,
        out_specs=(P("ga", "gx", "gy", "col"), P("ga", "col")),
        check_vma=False,
    )
```

```python
import functools

import jax
import jax.numpy as jnp
from jax import lax
from jax.experimental import pallas as pl
from jax.experimental.pallas import tpu as pltpu
from jax.sharding import PartitionSpec as P

epsilon = 1e-05
format_limit = 448.0
LANES = 128
F32 = jnp.float32
BF16 = jnp.bfloat16


def lane_round(size):
    return -(-size // LANES) * LANES


def normed_rows(rows, gain, bias):
    average = jnp.mean(rows, axis=-1, keepdims=True)
    spread = jnp.mean(jnp.square(rows - average), axis=-1, keepdims=True)
    return ((rows - average) * lax.rsqrt(spread + epsilon) * gain + bias).astype(BF16)


def one_hot_rows(channels, parity, dtype=BF16):
    row = lax.broadcasted_iota(jnp.int32, (2 * channels, channels), 0)
    col = lax.broadcasted_iota(jnp.int32, (2 * channels, channels), 1)
    return jnp.where(row == 2 * col + parity, 1.0, 0.0).astype(dtype)


def one_hot_cols(channels, parity):
    row = lax.broadcasted_iota(jnp.int32, (channels, 2 * channels), 0)
    col = lax.broadcasted_iota(jnp.int32, (channels, 2 * channels), 1)
    return jnp.where(col == 2 * row + parity, 1.0, 0.0).astype(BF16)


def in_hbm(array):
    return pltpu.with_memory_space_constraint(array, pltpu.HBM)


def nn(left, right):
    return jnp.dot(left, right, preferred_element_type=F32)


def nt(left, right):
    return lax.dot_general(left, right, (((1,), (1,)), ((), ())), preferred_element_type=F32)


def split_parts(values):
    high = values.astype(BF16).astype(F32)
    middle = (values - high).astype(BF16).astype(F32)
    return high, middle, values - high - middle


def columns_of(rows, channels):
    parts = jnp.concatenate([*split_parts(rows), jnp.zeros_like(rows)], axis=0).astype(BF16)
    both = (one_hot_rows(channels, 0, F32) + one_hot_rows(channels, 1, F32)).astype(BF16)
    return columns_of_parts(parts, both)


def columns_of_parts(parts, both):
    columns = nt(both, parts)
    return columns[:, 0:2] + columns[:, 2:4] + columns[:, 4:6]


def fetch_kernel(
    half_ref,
    rep_hbm,
    mask_hbm,
    weight_hbm,
    history_hbm,
    gain_hbm,
    bias_hbm,
    packed_ref,
    rep_ref,
    mask_ref,
    affine_ref,
    hots_ref,
    weight_ref,
    history_ref,
    sems,
):
    which, outs, channels = weight_ref.shape
    held = rep_ref.shape[0]
    copies = [
        pltpu.make_async_copy(source, target, sems.at[at])
        for at, (source, target) in enumerate(
            (
                (weight_hbm, weight_ref),
                (history_hbm, history_ref),
                (rep_hbm.at[pl.ds(half_ref[0] * held, held)], rep_ref),
                (gain_hbm, affine_ref.at[pl.ds(0, 1)]),
                (bias_hbm, affine_ref.at[pl.ds(1, 1)]),
                (mask_hbm, mask_ref),
            )
        )
    ]
    for copy in copies:
        copy.start()
    for parity in range(2):
        hots_ref[parity] = one_hot_rows(channels, parity)
    for copy in copies[:2]:
        copy.wait()
    for at in range(which):
        packed_ref[at * outs : (at + 1) * outs, :] = weight_ref[at]
    history = history_ref[...]
    parts = jnp.concatenate([*split_parts(history), jnp.zeros_like(history)], axis=0)
    parts = jnp.concatenate([parts, jnp.zeros_like(parts)], axis=1)
    parts = jnp.concatenate([parts, jnp.zeros_like(parts)], axis=0)
    packed_ref[which * outs :, :] = parts.astype(BF16)
    for copy in copies[2:]:
        copy.wait()


def history_parts(packed_ref, outs):
    start = packed_ref.shape[1] - 16
    pieces = [packed_ref[col, start:, :][:, :outs] for col in range(2)]
    return jnp.concatenate(pieces, axis=1)[:8]


def project_kernel(
    half_ref, packed_ref, rep_ref, mask_ref, affine_ref, hots_ref, out_hbm, near, far, proj, inverse_ref, out_ref, sems
):
    held, cols, channels = rep_ref.shape
    deep = held // 2
    span = deep * cols
    wide = near.shape[0]
    shift = span - (wide - LANES)
    near[pl.ds(span, wide - span), :] = jnp.zeros((wide - span, 2 * channels), BF16)
    far[pl.ds(0, shift), :] = jnp.zeros((shift, 2 * channels), BF16)
    far[pl.ds(shift + span, wide - span - shift), :] = jnp.zeros((wide - span - shift, 2 * channels), BF16)
    gain, bias = affine_ref[0:1, :], affine_ref[1:2, :]
    for part in range(2):
        block = rep_ref[part * deep : (part + 1) * deep].reshape(span, channels)
        block = normed_rows(block.astype(F32), gain, bias)
        lanes = slice(part * channels, (part + 1) * channels)
        near[0:span, lanes] = block
        far[shift : shift + span, lanes] = block
    masks = mask_ref[...].astype(F32)
    masks = jnp.where(half_ref[0] == 0, masks[:held], masks[held:])
    pieces = [
        jnp.concatenate([masks[at : at + 1], masks[deep + at : deep + at + 1]], axis=0)
        for at in range(deep)
    ]
    zeros = jnp.zeros((2, wide - span), F32)
    mask_near = jnp.concatenate([jnp.concatenate([*pieces, zeros], axis=1)] * 4, axis=0)
    mask_far = jnp.concatenate([pltpu.roll(mask_near, shift, 1)] * 2, axis=0)
    mask_near = jnp.concatenate([mask_near] * 2, axis=0)
    outs = channels // 2
    even, odd = hots_ref[0], hots_ref[1]
    inverse_ref[...] = format_limit / columns_of_parts(history_parts(packed_ref, outs), even + odd)
    weight = jnp.concatenate(
        [
            jnp.concatenate([packed_ref[0, at * outs : (at + 1) * outs], packed_ref[1, at * outs : (at + 1) * outs]], axis=0)
            for at in range(4)
        ],
        axis=1,
    )
    evens, odds = nn(even, weight).astype(BF16), nn(odd, weight).astype(BF16)
    for side in range(2):
        both = [
            jnp.concatenate([held[:, at * channels : (at + 1) * channels] for held in (evens, odds)], axis=1)
            for at in (2 * side, 2 * side + 1)
        ]
        values = nt(jnp.concatenate(both, axis=0), (near if side == 0 else far)[...])
        proj[2 * side : 2 * side + 2] = values.reshape(2, 2 * channels, wide)
    lane = lax.broadcasted_iota(jnp.int32, (16, LANES), 1)
    first = shift + span - (wide - LANES)

    def step(at, carry):
        rows_at = pl.ds(pl.multiple_of(at * 16, 16), 16)
        left = mask_near * jax.nn.sigmoid(proj[1, rows_at, :]) * proj[0, rows_at, :]
        right = mask_far * jax.nn.sigmoid(proj[3, rows_at, :]) * proj[2, rows_at, :]
        left_max = jnp.max(jnp.abs(left), axis=1, keepdims=True)
        right_max = jnp.max(jnp.abs(right), axis=1, keepdims=True)
        inverse = inverse_ref[rows_at, :]
        left = jnp.clip(left * inverse[:, 0:1], -format_limit, format_limit)
        right = jnp.clip(right * inverse[:, 1:2], -format_limit, format_limit)
        edge = wide - LANES
        peers_at = pl.ds(at * 8, 8)

        def put(start, stop, values):
            out_ref[peers_at, :, start:stop] = values.astype(BF16).reshape(8, 2, stop - start)

        put(0, edge, left[:, :edge])
        put(edge, wide, left[:, edge:] + right[:, :LANES])
        put(wide, wide + edge - LANES, right[:, LANES:edge])
        last = right[:, edge:]
        for place, part in enumerate((*split_parts(left_max), *split_parts(right_max))):
            last = jnp.where(lane == first + place, part, last)
        put(wide + edge - LANES, wide + edge, last)
        sent(at).start()
        return carry

    def sent(at):
        peers_at = pl.ds(at * 8, 8)
        return pltpu.make_async_copy(out_ref.at[peers_at], out_hbm.at[peers_at], sems.at[at])

    def settle(at, carry):
        sent(at).wait()
        return carry

    lax.fori_loop(0, channels // 8, step, 0, unroll=8)
    lax.fori_loop(0, channels // 8, settle, 0)


def gate_kernel(
    half_ref,
    mine_ref,
    rep_ref,
    packed_ref,
    gate_ref,
    weight_ref,
    gain_ref,
    bias_ref,
    affine_ref,
    gating_ref,
    mixer_ref,
    order_ref,
    columns_ref,
    scale_ref,
    chosen_ref,
    near,
):
    rows, cols, channels = rep_ref.shape
    deep = rows // 4
    span = deep * cols
    outs = gate_ref.shape[0]
    gain, bias = gain_ref[...], bias_ref[...]
    blank = jnp.zeros((outs, channels), BF16)
    gate = gate_ref[...]
    wide_gate = jnp.concatenate(
        [jnp.concatenate([gate, blank], axis=1), jnp.concatenate([blank, gate], axis=1)], axis=0
    )
    near[span:, :] = jnp.zeros((near.shape[0] - span, 2 * channels), BF16)
    for half in range(2):
        for part in range(2):
            start = half * (2 * deep) + part * deep
            block = rep_ref[start : start + deep].reshape(span, channels).astype(F32)
            near[0:span, part * channels : (part + 1) * channels] = normed_rows(block, gain, bias)
        gating_ref[half] = jax.nn.sigmoid(nt(wide_gate, near[...]))
    row = lax.broadcasted_iota(jnp.int32, chosen_ref.shape, 0)
    col = lax.broadcasted_iota(jnp.int32, chosen_ref.shape, 1)
    chosen_ref[...] = jnp.where(row == 2 * (col + half_ref[0] * outs), 1.0, 0.0).astype(BF16)
    columns_ref[...] = columns_of(affine_ref[...], channels)
    parts = history_parts(packed_ref, outs).astype(F32)
    lane = lax.broadcasted_iota(jnp.int32, parts.shape, 1)
    parts = jnp.sum(jnp.where(lane == mine_ref[0], parts, 0.0), axis=1, keepdims=True)
    scales = (parts[0:2] + parts[2:4] + parts[4:6]) / format_limit
    scale_ref[...] = jnp.broadcast_to(scales[0:1] * scales[1:2], scale_ref.shape)
    weight = weight_ref[...]
    mixer_ref[0:outs, :] = nn(weight, one_hot_cols(channels, 0)).astype(BF16)
    mixer_ref[outs:, :] = nn(weight, one_hot_cols(channels, 1)).astype(BF16)
    count, lanes = order_ref.shape
    per_half = count // 2
    per_at = per_half // deep
    pairs = cols // rows
    step = 32
    for start in range(0, count, step):
        row = start + lax.broadcasted_iota(jnp.int32, (step, 1), 0)
        half_at = start // per_half
        deep_at = (start % per_half) // per_at
        block = (row - half_at * per_half - deep_at * per_at) >> 1
        part = row & 1
        target = (block // pairs) * LANES + (block % pairs) * rows + half_at * 2 * deep + part * deep + deep_at
        lane = lax.broadcasted_iota(jnp.int32, (step, lanes), 1)
        order_ref[start : start + step, :] = jnp.where(lane == target, 1.0, 0.0).astype(BF16)


def unpack_kernel(received_ref, left_ref, right_ref, flat, *, groups, deep, cols):
    rows, lanes = flat.shape
    block = rows // groups
    span = deep * cols
    for group in range(groups):
        piece = received_ref[group * block // 2 : (group + 1) * block // 2]
        flat[group * block : (group + 1) * block, :] = piece.reshape(block, lanes)

    def window(group, start):
        base = start // LANES * LANES
        stop = -(-(start + cols) // LANES) * LANES
        return flat[group * block : (group + 1) * block, base:stop][:, start - base : start - base + cols]

    for at in range(deep):
        place = pl.ds(at * block, block)
        left_ref[place, :] = jnp.concatenate([window(g, at * cols) for g in range(groups)], axis=1)
        right_ref[place, :] = jnp.concatenate([window(g, span + at * cols) for g in range(groups)], axis=1)
    parts = flat[:, lanes - LANES :].astype(F32)
    total = parts + pltpu.roll(parts, LANES - 1, 1) + pltpu.roll(parts, LANES - 2, 1)
    best = jnp.max(jnp.max(total.reshape(rows // 8, 8, LANES), axis=0), axis=0, keepdims=True)
    best = jnp.concatenate([*split_parts(best), jnp.zeros((13, LANES), F32)], axis=0).astype(BF16)
    right_ref[deep * block :, :] = jnp.concatenate(
        [best, jnp.zeros((16, groups * cols - LANES), BF16)], axis=1
    )


def triangle_kernel(scale_ref, left_ref, both_ref, order_ref, out_ref, moved, *, groups, deep, cols):
    count = left_ref.shape[0]
    block = count // deep
    span = deep * cols
    scale = scale_ref[0:1, 0:1]
    best = None
    for other in range(2):
        parts = both_ref[other, count:, :LANES].astype(F32)
        parts = parts[0:1] + parts[1:2] + parts[2:3]
        best = parts if best is None else jnp.maximum(best, parts)
    right = jnp.concatenate([both_ref[other, :count, :] for other in range(2)], axis=0)
    products = nt(left_ref[...], right) * scale
    moved[...] = nn(products.astype(BF16), order_ref[...]).astype(BF16)
    lane = lax.broadcasted_iota(jnp.int32, (8, LANES), 1)
    first = 2 * span % LANES
    goal = span % LANES
    best = jnp.broadcast_to(best, (8, LANES))
    tail = jnp.zeros((8, LANES), F32)
    for place, part in enumerate(split_parts(best)):
        turned = pltpu.roll(part, (goal + place - first) % LANES, 1)
        tail = jnp.where((lane == goal + place) | (lane == goal + place + 3), turned, tail)
    tail = jnp.broadcast_to(tail[0:1, goal:], (block, LANES - goal)).astype(BF16)
    for group in range(groups):
        pieces = [
            moved[at * block : (at + 1) * block, group * LANES : group * LANES + cols] for at in range(deep)
        ]
        pieces = jnp.concatenate([*pieces, tail], axis=1)
        out_ref[group * block // 2 : (group + 1) * block // 2] = pieces.reshape(block // 2, 2, -1)


def finish_kernel(
    both_ref, gating_ref, mixer_ref, columns_ref, chosen_ref, update_ref, amax_ref, mixed, *, deep, cols
):
    rows, wide = both_ref.shape[1:]
    channels = rows // 2
    outs = update_ref.shape[1]
    span = deep * cols
    gain, bias = columns_ref[:, 0:1], columns_ref[:, 1:2]
    mixer = mixer_ref[...]

    def per_part(values):
        total = jnp.sum(values, axis=0)
        total = total + pltpu.roll(total, 4, 0)
        total = total + pltpu.roll(total, 2, 0)
        return total * (1.0 / channels)

    for half in range(2):
        for start in range(0, wide, LANES):
            values = both_ref[half, :, start : start + LANES].astype(F32).reshape(rows // 8, 8, LANES)
            values = values - per_part(values)[None]
            spread = per_part(jnp.square(values))
            values = (values * lax.rsqrt(spread + epsilon)[None]).reshape(rows, LANES)
            tnorm = (values * gain + bias).astype(BF16)
            mixing = nn(mixer, tnorm)
            mixed[:, start : start + LANES] = (gating_ref[half, :, start : start + LANES] * mixing).astype(BF16)
        for part in range(2):
            for at in range(deep):
                place = half * 2 * deep + part * deep + at
                update_ref[place] = mixed[part * outs : (part + 1) * outs, at * cols : (at + 1) * cols]
    last = both_ref[0, :, wide - LANES :]
    sums = lax.dot_general(last, chosen_ref[...], (((0,), (0,)), ((), ())), preferred_element_type=F32)
    goal = span % LANES
    amax_ref[0:1, :] = sums[goal : goal + 1] + sums[goal + 1 : goal + 2] + sums[goal + 2 : goal + 3]
    amax_ref[1:2, :] = sums[goal + 3 : goal + 4] + sums[goal + 4 : goal + 5] + sums[goal + 5 : goal + 6]


VMEM = pl.BlockSpec(memory_space=pltpu.VMEM)
HBM = pl.BlockSpec(memory_space=pltpu.HBM)
SMEM = pl.BlockSpec(memory_space=pltpu.SMEM)
GRANT = pltpu.CompilerParams(vmem_limit_bytes=24 * 2**20)


def on_device(
    pair_rep,
    pair_mask,
    amax_history,
    in_gain,
    in_bias,
    proj_weight,
    gate_weight,
    out_gain,
    out_bias,
    out_weight,
):
    rows, cols, channels = pair_rep.shape[1:]
    deep = rows // 4
    span = deep * cols
    wide = lane_round(span)
    groups, ranks = lax.axis_size("gy"), lax.axis_size("gx")
    chips = ("gy", "gx")
    assert groups * ranks == channels and lax.axis_size("col") == 2
    half = lax.axis_index("col").reshape(1).astype(jnp.int32)
    rep = pair_rep[0]
    gain, bias = in_gain[None, :], in_bias[None, :]

    packed, held, mask, affine, hots = pl.pallas_call(
        fetch_kernel,
        name="fetch",
        out_shape=(
            jax.ShapeDtypeStruct((2 * channels + 16, channels), BF16),
            jax.ShapeDtypeStruct((rows // 2, cols, channels), BF16),
            jax.ShapeDtypeStruct((rows, cols), jnp.int32),
            jax.ShapeDtypeStruct((2, channels), F32),
            jax.ShapeDtypeStruct((2, 2 * channels, channels), BF16),
        ),
        in_specs=[SMEM] + [HBM] * 6,
        out_specs=(VMEM,) * 5,
        scratch_shapes=[
            pltpu.VMEM((4, channels // 2, channels), BF16),
            pltpu.VMEM((2, channels // 2), F32),
            pltpu.SemaphoreType.DMA((6,)),
        ],
        compiler_params=GRANT,
    )(half, *map(in_hbm, (rep, pair_mask[0], jnp.transpose(proj_weight, (1, 2, 0)), amax_history, gain, bias)))
    packed = lax.all_gather(packed, "col")
    message = pl.pallas_call(
        project_kernel,
        name="project",
        out_shape=pltpu.HBM((channels, 2, 2 * wide - LANES), BF16),
        in_specs=[SMEM] + [VMEM] * 5,
        out_specs=HBM,
        scratch_shapes=[
            pltpu.VMEM((wide, 2 * channels), BF16),
            pltpu.VMEM((wide, 2 * channels), BF16),
            pltpu.VMEM((4, 2 * channels, wide), F32),
            pltpu.VMEM((2 * channels, 2), F32),
            pltpu.VMEM((channels, 2, 2 * wide - LANES), BF16),
            pltpu.SemaphoreType.DMA((channels // 8,)),
        ],
        compiler_params=GRANT,
    )(half, packed, held, mask, affine, hots)
    received = lax.all_to_all(message, chips, split_axis=0, concat_axis=0, tiled=True)
    mine = lax.axis_index(chips).reshape(1).astype(jnp.int32)
    gating, mixer, order, columns, scale, chosen = pl.pallas_call(
        gate_kernel,
        name="gate",
        out_shape=(
            jax.ShapeDtypeStruct((2, channels, wide), F32),
            jax.ShapeDtypeStruct((channels, 2 * channels), BF16),
            jax.ShapeDtypeStruct((ranks * rows, groups * LANES), BF16),
            jax.ShapeDtypeStruct((2 * channels, 2), F32),
            jax.ShapeDtypeStruct((8, LANES), F32),
            jax.ShapeDtypeStruct((2 * channels, channels // 2), BF16),
        ),
        in_specs=[SMEM] * 2 + [VMEM] * 7,
        out_specs=(VMEM,) * 6,
        scratch_shapes=[pltpu.VMEM((wide, 2 * channels), BF16)],
        compiler_params=GRANT,
        cost_estimate=pl.CostEstimate(flops=20_000_000_000, bytes_accessed=3_000_000, transcendentals=0),
    )(half, mine, rep, packed, gate_weight.T, out_weight.T, gain, bias, jnp.stack([out_gain, out_bias]))
    count = ranks * rows // 2
    left, right = pl.pallas_call(
        functools.partial(unpack_kernel, groups=groups, deep=deep, cols=cols),
        name="unpack",
        out_shape=(
            jax.ShapeDtypeStruct((count, groups * cols), BF16),
            jax.ShapeDtypeStruct((count + 16, groups * cols), BF16),
        ),
        in_specs=[VMEM],
        out_specs=(VMEM,) * 2,
        scratch_shapes=[pltpu.VMEM((2 * channels, 2 * wide - LANES), BF16)],
        compiler_params=GRANT,
    )(received)
    both = lax.all_gather(right, "col")
    products = pl.pallas_call(
        functools.partial(triangle_kernel, groups=groups, deep=deep, cols=cols),
        name="triangle",
        out_shape=jax.ShapeDtypeStruct((channels, 2, wide), BF16),
        in_specs=[VMEM] * 4,
        out_specs=VMEM,
        scratch_shapes=[pltpu.VMEM((count, groups * LANES), BF16)],
        compiler_params=GRANT,
    )(scale, left, both, order)
    returned = lax.all_to_all(products, chips, split_axis=0, concat_axis=0, tiled=True)
    both = lax.all_gather(returned.reshape(2 * channels, -1), "col")
    update, new_amax = pl.pallas_call(
        functools.partial(finish_kernel, deep=deep, cols=cols),
        name="finish",
        out_shape=(
            jax.ShapeDtypeStruct((rows, channels // 2, cols), BF16),
            jax.ShapeDtypeStruct((2, channels // 2), F32),
        ),
        in_specs=[VMEM] * 5,
        out_specs=(VMEM,) * 2,
        scratch_shapes=[pltpu.VMEM((channels, wide), BF16)],
        compiler_params=GRANT,
    )(both, gating, mixer, columns, chosen)
    return (jnp.transpose(update, (0, 2, 1))[None], new_amax)


def solution(mesh):
    placed = (
        P("ga", "gx", "gy", None),
        P("ga", "gx", "gy"),
        P(None, "col"),
        P(),
        P(),
        P(None, None, "col"),
        P(None, "col"),
        P(),
        P(),
        P(None, "col"),
    )
    return jax.shard_map(
        on_device,
        mesh=mesh,
        in_specs=placed,
        out_specs=(P("ga", "gx", "gy", "col"), P("ga", "col")),
        check_vma=False,
    )
```
